512 devices in a mesh: rep: 8 (over x, core), shard: 64 (over z, y).
Axes of the slice: x: 4, y: 8, z: 8, core: 2. Of those that a mesh axis runs over, the one named last changes fastest.
Arguments:
- features: float32 [262144, 256], P(('rep', 'shard')), may hold values from -6 to 6
- seed_self: float32 [65536, 256], P(('rep', 'shard')), may hold values from -6 to 6
- hub_ids: int32 [65536], P(('rep', 'shard')), may hold values from 0 to 511
- requests: int32 [32768, 32], P(('rep', 'shard')), may hold values from 0 to 511
- counts: int32 [32768], P(('rep', 'shard')), may hold values from 1 to 32, as said below
- neighbors: int32 [65536, 15], P(('rep', 'shard')), may hold values from 0 to 3071
- weight: float32 [256, 256], replicated, may hold values from -1 to 1
- out_bias: float32 [256], replicated, may hold values from -4 to 4
Outputs:
- embedded: float32 [65536, 256], P(('rep', 'shard'))
The draws below stay inside these ranges and needn't reach their ends.
Inputs may be any that keep to these rules, and one draw needn't show every extreme that they name: `hub_ids`: offsets into the block of features of the same device. `requests`: row d of a device's lists holds offsets into the block of features of the device at shard index d with the same rep index; empty slots hold offsets too. counts[r, s, d] slots of the list from shard index s to shard index d are live, the first ones; for every rep index some destination has 32 live slots from every source. `neighbors`: A code below 1024 names a row of the device's hub cache; a code 1024 + d * 32 + c names slot c of the device's list to shard index d, and counts only where that slot is live.
All inputs are finite; a program needn't handle non-finite values.
Results may differ from the reference program's by a relative error of at most 0.0003.
Values sent between devices are 32-bit elements; how exact they have to be, the bound alone decides.
A program may use at most 64 MiB of HBM per device.

```python
import jax
import jax.numpy as jnp
from jax import lax

F = 256
FANOUT = 15
CAP = 32
ROWS_DEV = 512
SEEDS_DEV = 128
HUB_DEV = 128
HUBS = 1024
SLOTS_DEV = 2048
CODES = 3072
NODES = 262144
SEEDS = 65536
HUB_SLOTS = 65536
REQ_ROWS = 32768
N_REP = 8
N_SHARD = 64


def draw_counts(key, part):
    k_base, k_owner = jax.random.split(jax.random.fold_in(key, 11), 2)
    base_fill = jax.random.randint(k_base, (N_REP, N_SHARD, N_SHARD), CAP // 4, CAP + 1)
    full_owner = jax.random.randint(k_owner, (N_REP, 1, 1), 0, N_SHARD)
    owner_index = lax.broadcasted_iota(jnp.int32, (N_REP, N_SHARD, N_SHARD), 2)
    result = jnp.where(owner_index == full_owner, CAP, base_fill)
    return result.reshape(-1).astype(jnp.int32)


def plant(entries, rng, low, top_value):
    longest = entries.shape.index(max(entries.shape))
    spots = []
    for shift in (0, 1):
        where = [jax.random.randint(jax.random.fold_in(rng, axis), (), 0, length) for axis, length in enumerate(entries.shape)]
        where[longest] = (where[longest] + shift) % entries.shape[longest]
        spots.append(tuple(where))
    return entries.at[spots[0]].set(low).at[spots[1]].set(top_value)


def steps_of(stream_key, extent, shards, low, largest):
    gain = 1.0
    for position, parts in shards:
        steps = jax.random.uniform(jax.random.fold_in(jax.random.fold_in(stream_key, 6), position), (parts,), jnp.float32, low / len(shards), largest / len(shards))
        gain = gain * jnp.repeat(jnp.exp(steps), extent[position] // parts).reshape((-1,) + (1,) * (len(extent) - 1 - position))
    return gain


def bell_draw(rng, extent, deviation, bound, cuts=(), kind=jnp.bfloat16):
    level = steps_of(rng, extent, cuts, -0.22, 0.18) if cuts else 1.0
    values = jax.random.normal(rng, extent, jnp.float32) * deviation * level
    return jnp.minimum(jnp.maximum(values, -bound), bound).astype(kind)


def setup_inputs(seed: int = 0) -> dict:
    seeds = jax.random.split(jax.random.key(seed), 9)
    features = bell_draw(seeds[0], (NODES, F), 1.0, 6.0, ((0, 512),), jnp.float32)
    seed_self = bell_draw(seeds[1], (SEEDS, F), 1.0, 6.0, ((0, 512),), jnp.float32)
    hub_ids = plant(jax.random.randint(seeds[2], (HUB_SLOTS,), 0, ROWS_DEV), jax.random.fold_in(seeds[2], 1), 0, ROWS_DEV - 1).astype(jnp.int32)
    requests = plant(jax.random.randint(seeds[3], (REQ_ROWS, CAP), 0, ROWS_DEV), jax.random.fold_in(seeds[3], 1), 0, ROWS_DEV - 1).astype(jnp.int32)
    counts = draw_counts(jax.random.fold_in(seeds[8], 71), 0)
    neighbors = plant(jax.random.randint(seeds[5], (SEEDS, FANOUT), 0, CODES), jax.random.fold_in(seeds[5], 1), 0, CODES - 1).astype(jnp.int32)
    weight = bell_draw(seeds[6], (F, F), (F // 8) ** -0.5, 1.0, (), jnp.float32)
    out_bias = bell_draw(seeds[7], (F,), 1.0, 4.0, (), jnp.float32)
    return dict(features=features, seed_self=seed_self, hub_ids=hub_ids, requests=requests, counts=counts, neighbors=neighbors, weight=weight, out_bias=out_bias)


def reference(features, seed_self, hub_ids, requests, counts, neighbors, weight, out_bias):
    blocks = features.reshape(N_REP, N_SHARD, ROWS_DEV, F)
    hub_index = hub_ids.reshape(N_REP, N_SHARD, HUB_DEV)
    request_index = requests.reshape(N_REP, N_SHARD, N_SHARD, CAP)
    fill_counts = counts.reshape(N_REP, N_SHARD, N_SHARD)
    neighbor_codes = neighbors.reshape(N_REP * N_SHARD, SEEDS_DEV, FANOUT)
    own_rows = seed_self.reshape(N_REP * N_SHARD, SEEDS_DEV, F)
    rep_iota = jnp.arange(N_REP, dtype=jnp.int32)[:, None]
    shard_iota = jnp.arange(N_SHARD, dtype=jnp.int32)[:, None]
    slot_iota = jnp.arange(CAP, dtype=jnp.int32)[None, :]

    def per_device(device_index):
        rep_pos = device_index // N_SHARD
        shard_pos = device_index % N_SHARD
        hub_cache = blocks[rep_iota, shard_pos, hub_index[:, shard_pos]].reshape(HUBS, F)
        fetched = blocks[rep_pos, shard_iota, request_index[rep_pos, shard_pos]].reshape(SLOTS_DEV, F)
        source = jnp.concatenate([hub_cache, fetched], axis=0)
        slot_live = (slot_iota < fill_counts[rep_pos, shard_pos][:, None]).astype(jnp.float32)
        live = jnp.concatenate([jnp.ones((HUBS,), jnp.float32), slot_live.reshape(SLOTS_DEV)])
        codes = neighbor_codes[device_index]
        picked = source[codes]
        weights = live[codes]
        total = own_rows[device_index] + jnp.sum(picked * weights[:, :, None], axis=1)
        taken = 1.0 + jnp.sum(weights, axis=1)
        mean_rows = total / taken[:, None]
        product = jnp.dot(mean_rows, weight, precision=lax.Precision.HIGHEST, preferred_element_type=jnp.float32)
        return jnp.maximum(product + out_bias, 0.0)

    result = lax.map(per_device, jnp.arange(N_REP * N_SHARD, dtype=jnp.int32))
    return result.reshape(SEEDS, F)
```

```python
import functools

import jax
import jax.numpy as jnp
from jax import lax
from jax.experimental import pallas as pl
from jax.experimental.pallas import tpu as pltpu
from jax.sharding import PartitionSpec as P

MESH = pl.DeviceIdType.MESH
RING = 8
XS = 4
ROWS = 512
SEEDS = 128
FAN = 15
CAP = 32
HUBS = 1024
CHUNKS = 4
LANES = 128


def split(values):
    high = values.astype(jnp.bfloat16)
    low = (values - high.astype(jnp.float32)).astype(jnp.bfloat16)
    return jnp.concatenate([high, low], axis=0)


def dot(left, right):
    return jnp.dot(left, right, preferred_element_type=jnp.float32)


def kernel(
    feat, own, hub_id, req, req_t, counts, codes_t, weight, bias, out,
    ag, meta_tx, meta_rx, ids, cblk, gacc, pacc, part, hubs, tot, taken,
    ag_send, ag_recv, meta_send, meta_recv, part_send, part_recv, hub_send, hub_recv,
):
    rep = lax.axis_index("rep")
    shard = lax.axis_index("shard")
    me_x, core = rep // 2, rep % 2
    me = (shard % RING, shard // RING)

    def along_y(step):
        return {"rep": rep, "shard": me[1] * RING + (me[0] + step) % RING}

    def along_z(step):
        return {"rep": rep, "shard": ((me[1] + step) % RING) * RING + me[0]}

    def along_x(step):
        return {"rep": ((me_x + step) % XS) * 2 + core, "shard": shard}

    ring = (along_y, along_z)
    cross = (along_z, along_y)
    spot = (me[1], me[0])

    barrier = pltpu.get_barrier_semaphore()
    peers = [along_y(d) for d in range(1, RING)] + [along_z(d) for d in range(1, RING)]
    partner = {"rep": me_x * 2 + 1 - core, "shard": shard}
    peers += [partner, along_x(1), along_x(XS - 1)]
    for peer in peers:
        pl.semaphore_signal(barrier, inc=1, device_id=peer, device_id_type=MESH)

    def push(src, dst, send, recv, peer):
        return pltpu.make_async_remote_copy(
            src_ref=src, dst_ref=dst, send_sem=send, recv_sem=recv, device_id=peer, device_id_type=MESH
        )

    for half in range(2):
        for chunk in range(CHUNKS):
            block = feat[chunk * LANES : (chunk + 1) * LANES, half * LANES : (half + 1) * LANES]
            ag[half, 0, chunk] = jnp.transpose(block)

    codes = codes_t[...]
    owner = (codes - HUBS) >> 5
    slot = (codes - HUBS) & 31

    def look(d, found):
        return jnp.where(owner == d, counts[d], found)

    filled = lax.fori_loop(0, RING * RING, look, jnp.zeros_like(codes), unroll=8)
    live = (codes >= 0) & ((codes < HUBS) | (slot < filled))
    codes = jnp.where(live, codes, -1)
    taken[...] = 1.0 + jnp.sum(live.astype(jnp.float32), axis=0, keepdims=True)
    for half, source in enumerate((req, req_t)):
        turned = pltpu.roll(source[...], (spot[half] % 4) * CAP, 1)
        for place in range(RING):
            meta_tx[half, place, 0:16] = codes
            meta_tx[half, place, 16:24] = turned[place * RING : (place + 1) * RING]
        meta_rx[half, spot[half], 0:16] = codes
    for half in range(2):
        meta_rx[half, spot[half], 16:24] = meta_tx[half, spot[half], 16:24]

    hub_sum = jnp.zeros((4 * LANES, LANES), jnp.float32)
    for chunk in range(CHUNKS):
        block = jnp.concatenate([ag[0, 0, chunk], ag[1, 0, chunk]], axis=0)
        rows = lax.broadcasted_iota(jnp.int32, (LANES, LANES), 0) + chunk * LANES
        pick = jnp.where(rows == hub_id[...], 1.0, 0.0).astype(jnp.bfloat16)
        hub_sum = hub_sum + dot(split(block), pick)
    hubs[0] = hub_sum[: 2 * LANES] + hub_sum[2 * LANES :]

    pl.semaphore_wait(barrier, len(peers))

    sent = []

    def launch(copy):
        copy.start()
        sent.append(copy)

    metas = []
    for step in (4, 3, 5, 2, 6, 1, 7):
        for half in range(2):
            place = (spot[half] + step) % RING
            copy = push(
                meta_tx.at[half, place], meta_rx.at[half, spot[half]],
                meta_send.at[half, step - 1], meta_recv.at[half, step - 1], cross[half](step),
            )
            launch(copy)
            metas.append(copy)

    def table(half, way, wave, chunk):
        slot_from = wave if way == 0 else (RING - wave) % RING
        slot_to = wave + 1 if way == 0 else RING - wave - 1
        return push(
            ag.at[half, slot_from, chunk], ag.at[half, slot_to, chunk],
            ag_send.at[half, way, wave, chunk], ag_recv.at[half, slot_to, chunk],
            ring[half](1 if way == 0 else RING - 1),
        )

    moves = {}
    for chunk in range(CHUNKS):
        for half in range(2):
            for way in range(2):
                moves[half, way, 0, chunk] = table(half, way, 0, chunk)
                launch(moves[half, way, 0, chunk])

    def hub_push(index, src, dst, peer):
        copy = push(src, dst, hub_send.at[index], hub_recv.at[index], peer)
        launch(copy)
        return copy

    hub_right = hub_push(0, hubs.at[0], hubs.at[2], along_x(1))
    hub_left = hub_push(1, hubs.at[0], hubs.at[6], along_x(XS - 1))
    hub_over = [hub_push(2, hubs.at[0], hubs.at[1], partner)]

    cblk[...] = jnp.zeros_like(cblk)
    pacc[...] = jnp.zeros_like(pacc)
    tot[...] = jnp.transpose(own[...])

    for copy in metas:
        copy.wait_recv()
    for half in range(2):
        for group in range(2):
            tiles = [meta_rx[half, 4 * group + k, 16:24] for k in range(4)]
            ids[half, :, group * LANES : (group + 1) * LANES] = tiles[0] + tiles[1] + tiles[2] + tiles[3]

    def place_of(half, slot_index):
        mine = me[0] * (1 - half) + me[1] * half
        return (mine + RING - slot_index) % RING

    def pick_rows(half, slot_index, part_index):
        pieces = [ag[half, slot_index, 2 * part_index + k] for k in range(2)]
        block = split(jnp.concatenate(pieces, axis=1))
        wanted = ids[half, pl.ds(place_of(half, slot_index), 1), :]
        rows = lax.broadcasted_iota(jnp.int32, (2 * LANES, 2 * LANES), 0) + 2 * LANES * part_index
        return dot(block, jnp.where(rows == wanted, 1.0, 0.0).astype(jnp.bfloat16))

    def add_seeds(half, slot_index, rows):
        origin = place_of(half, slot_index)
        number = origin * (1 + half * (RING - 1)) + (me[1] * RING) * (1 - half) + me[0] * half
        lines = lax.broadcasted_iota(jnp.int32, (CAP, LANES), 0) + (HUBS + number * CAP)
        for place in range(RING):
            count = jnp.zeros((CAP, LANES), jnp.float32)
            for k in range(FAN):
                count = count + jnp.where(meta_rx[half, place, k : k + 1] == lines, 1.0, 0.0)
            top, left = CAP * (place % 4), LANES * (place % 2)
            cblk[place // 2, top : top + CAP, left : left + LANES] = count.astype(jnp.bfloat16)
        rows = rows.astype(jnp.bfloat16)
        for pair in range(RING // 2):
            side = (pair // 2) * LANES
            sums = dot(rows[:, side : side + LANES], cblk[pair])
            sums = sums[:LANES] + sums[LANES:]
            for k in range(2):
                pacc[half, 2 * pair + k] += sums[:, k * LANES : (k + 1) * LANES]

    def own_block(half, carry):
        add_seeds(half, 0, pick_rows(half, 0, 0) + pick_rows(half, 0, 1))
        return carry

    lax.fori_loop(0, 2, own_block, 0)

    def first_part(wave, index, carry):
        half, way = index // 2, index % 2
        slot_index = wave + way * (RING - 2 * wave)
        gacc[index] = pick_rows(half, slot_index, 0)
        return carry

    def second_part(wave, index, carry):
        half, way = index // 2, index % 2
        slot_index = wave + way * (RING - 2 * wave)
        add_seeds(half, slot_index, gacc[index] + pick_rows(half, slot_index, 1))
        return carry

    def hub_block(index, carry):
        chip, over = index // 2, index % 2
        origin = ((me_x + XS - chip) % XS) * 2 + (core + over) % 2
        lines = lax.broadcasted_iota(jnp.int32, (LANES, LANES), 0) + origin * LANES
        mine = spot[0]
        count = jnp.zeros((LANES, LANES), jnp.float32)
        for k in range(FAN):
            count = count + jnp.where(meta_rx[0, mine, k : k + 1] == lines, 1.0, 0.0)
        sums = dot(split(hubs[index]), count.astype(jnp.bfloat16))
        tot[...] += sums[: 2 * LANES] + sums[2 * LANES :]
        return carry

    for wave in range(1, 4):
        for chunk in range(CHUNKS):
            for half in range(2):
                for way in range(2):
                    moves[half, way, wave - 1, chunk].wait_recv()
                    if wave < 3 or chunk // 2 == way:
                        moves[half, way, wave, chunk] = table(half, way, wave, chunk)
                        launch(moves[half, way, wave, chunk])
            if chunk == 1:
                lax.fori_loop(0, 4, functools.partial(first_part, wave), 0)
            if chunk == 3:
                lax.fori_loop(0, 4, functools.partial(second_part, wave), 0)
        if wave == 1:
            hub_right.wait_recv()
            hub_left.wait_recv()
            low, high = pl.ds(0, LANES), pl.ds(LANES, LANES)
            far = [
                hub_push(3, hubs.at[2, low], hubs.at[4, low], along_x(1)),
                hub_push(4, hubs.at[6, high], hubs.at[4, high], along_x(XS - 1)),
            ]
            hub_over.append(hub_push(5, hubs.at[2], hubs.at[3], partner))
            hub_over.append(hub_push(6, hubs.at[6], hubs.at[7], partner))
        if wave == 2:
            for copy in far:
                copy.wait_recv()
            hub_over.append(hub_push(7, hubs.at[4], hubs.at[5], partner))

    for copy in hub_over:
        copy.wait_recv()
    lax.fori_loop(0, 8, hub_block, 0)

    for chunk in (0, 2, 1, 3):
        for half in range(2):
            moves[half, chunk // 2, 3, chunk].wait_recv()

    sums_moves = []
    for half in range(2):
        add_seeds(half, 4, pick_rows(half, 4, 0) + pick_rows(half, 4, 1))
        for step in (4, 3, 5, 2, 6, 1, 7):
            copy = push(
                pacc.at[half, (spot[half] + step) % RING], part.at[half, step - 1],
                part_send.at[half, step - 1], part_recv.at[half, step - 1], cross[half](step),
            )
            launch(copy)
            sums_moves.append((half, step, copy))

    for half in range(2):
        tot[half * LANES : (half + 1) * LANES] += pacc[half, spot[half]]
    for wanted in (1, 7, 2, 6, 3, 5, 4):
        for half, step, copy in sums_moves:
            if step == wanted:
                copy.wait_recv()
                tot[half * LANES : (half + 1) * LANES] += part[half, step - 1]

    mean = jnp.transpose(tot[...] / taken[...])
    product = jnp.dot(mean, weight[...], precision=lax.Precision.HIGHEST, preferred_element_type=jnp.float32)
    out[...] = jnp.maximum(product + bias[...], 0.0)
    for copy in sent:
        copy.wait_send()


def local(features, seed_self, hub_ids, requests, counts, neighbors, weight, out_bias):
    codes_t = jnp.pad(neighbors.T, ((0, 16 - FAN), (0, 0)), constant_values=-1)
    req = jnp.pad(requests, ((0, 0), (0, LANES - CAP)))
    req_t = req.reshape(RING, RING, LANES).transpose(1, 0, 2).reshape(RING * RING, LANES)
    vmem = pl.BlockSpec(memory_space=pltpu.VMEM)
    smem = pl.BlockSpec(memory_space=pltpu.SMEM)
    dma = pltpu.SemaphoreType.DMA
    return pl.pallas_call(
        kernel,
        out_shape=jax.ShapeDtypeStruct((SEEDS, 2 * LANES), jnp.float32),
        in_specs=[vmem] * 5 + [smem] + [vmem] * 3,
        out_specs=vmem,
        scratch_shapes=[
            pltpu.VMEM((2, RING, CHUNKS, LANES, LANES), jnp.float32),
            pltpu.VMEM((2, RING, 24, LANES), jnp.int32),
            pltpu.VMEM((2, RING, 24, LANES), jnp.int32),
            pltpu.VMEM((2, RING, 2 * LANES), jnp.int32),
            pltpu.VMEM((4, LANES, 2 * LANES), jnp.bfloat16),
            pltpu.VMEM((4, 2 * LANES, 2 * LANES), jnp.float32),
            pltpu.VMEM((2, RING, LANES, LANES), jnp.float32),
            pltpu.VMEM((2, RING - 1, LANES, LANES), jnp.float32),
            pltpu.VMEM((2 * XS, 2 * LANES, LANES), jnp.float32),
            pltpu.VMEM((2 * LANES, LANES), jnp.float32),
            pltpu.VMEM((1, LANES), jnp.float32),
            dma((2, 2, 4, CHUNKS)),
            dma((2, RING, CHUNKS)),
            dma((2, RING - 1)),
            dma((2, RING - 1)),
            dma((2, RING - 1)),
            dma((2, RING - 1)),
            dma((8,)),
            dma((8,)),
        ],
        compiler_params=pltpu.CompilerParams(collective_id=0, has_side_effects=True, vmem_limit_bytes=48 * 1024 * 1024),
        name="sage",
    )(features, seed_self, hub_ids.reshape(1, LANES), req, req_t, counts, codes_t, weight, out_bias.reshape(1, 2 * LANES))


def solution(mesh):
    rows, flat = P(("rep", "shard"), None), P(("rep", "shard"))
    return jax.shard_map(
        local, mesh=mesh, in_specs=(rows, rows, flat, rows, flat, rows, P(), P()), out_specs=rows, check_vma=False
    )
```

```python
import functools

import jax
import jax.numpy as jnp
from jax import lax
from jax.experimental import pallas as pl
from jax.experimental.pallas import tpu as pltpu
from jax.sharding import PartitionSpec as P

MESH = pl.DeviceIdType.MESH
RING = 8
XS = 4
ROWS = 512
SEEDS = 128
FAN = 15
CAP = 32
HUBS = 1024
CHUNKS = 4
LANES = 128


def split(values):
    high = values.astype(jnp.bfloat16)
    low = (values - high.astype(jnp.float32)).astype(jnp.bfloat16)
    return jnp.concatenate([high, low], axis=0)


def dot(left, right):
    return jnp.dot(left, right, preferred_element_type=jnp.float32)


def kernel(
    feat_in, own_in, hub_in, req_in, counts_in, codes_in, weight_in, bias_in, out,
    feat, own, hub_id, req_v, req, counts, codes_v, weight, bias, fetch,
    ag, meta_tx, meta_rx, ids, cblk, gacc, pacc, part, hubs, tot, taken,
    ag_send, ag_recv, meta_send, meta_recv, part_send, part_recv, hub_send, hub_recv, token,
):
    rep = lax.axis_index("rep")
    shard = lax.axis_index("shard")
    me_x, core = rep // 2, rep % 2
    me = (shard % RING, shard // RING)

    def along_y(step):
        return {"rep": rep, "shard": me[1] * RING + (me[0] + step) % RING}

    def along_z(step):
        return {"rep": rep, "shard": ((me[1] + step) % RING) * RING + me[0]}

    def along_x(step):
        return {"rep": ((me_x + step) % XS) * 2 + core, "shard": shard}

    ring = (along_y, along_z)
    cross = (along_z, along_y)
    spot = (me[1], me[0])

    barrier = pltpu.get_barrier_semaphore()
    partner = {"rep": me_x * 2 + 1 - core, "shard": shard}
    peers = [along_y(1), along_y(RING - 1), along_z(1), along_z(RING - 1), along_x(1), along_x(XS - 1), partner]
    for peer in peers:
        pl.semaphore_signal(barrier, inc=1, device_id=peer, device_id_type=MESH)

    loads = []

    def load(src, dst):
        copy = pltpu.make_async_copy(src, dst, fetch.at[len(loads)])
        copy.start()
        loads.append(copy)
        return copy

    tables = [load(feat_in.at[pl.ds(c * LANES, LANES)], feat.at[pl.ds(c * LANES, LANES)]) for c in range(CHUNKS)]
    small = [load(codes_in, codes_v), load(counts_in, counts), load(req_in, req_v), load(hub_in, hub_id)]
    large = [load(own_in, own), load(weight_in, weight), load(bias_in, bias)]

    def push(src, dst, send, recv, peer):
        return pltpu.make_async_remote_copy(
            src_ref=src, dst_ref=dst, send_sem=send, recv_sem=recv, device_id=peer, device_id_type=MESH
        )

    sent = []

    def launch(copy):
        copy.start()
        sent.append(copy)

    def table(half, way, wave, chunk):
        slot_from = wave if way == 0 else (RING - wave) % RING
        slot_to = wave + 1 if way == 0 else RING - wave - 1
        return push(
            ag.at[half, slot_from, chunk], ag.at[half, slot_to, chunk],
            ag_send.at[half, way, wave, chunk], ag_recv.at[half, slot_to, chunk],
            ring[half](1 if way == 0 else RING - 1),
        )

    moves = {}

    def turn(chunk):
        tables[chunk].wait()
        for half in range(2):
            block = feat[chunk * LANES : (chunk + 1) * LANES, half * LANES : (half + 1) * LANES]
            ag[half, 0, chunk] = jnp.transpose(block)

    def send_own(chunk):
        for half in range(2):
            for way in range(2):
                moves[half, way, 0, chunk] = table(half, way, 0, chunk)
                launch(moves[half, way, 0, chunk])

    def tell(half, way):
        peer = ring[half](1 if way == 0 else RING - 1)
        pl.semaphore_signal(token.at[half, way], inc=1, device_id=peer, device_id_type=MESH)

    cblk[...] = jnp.zeros_like(cblk)
    pacc[...] = jnp.zeros_like(pacc)
    turn(0)
    pl.semaphore_wait(barrier, len(peers))
    for half in range(2):
        for way in range(2):
            tell(half, way)
    send_own(0)
    turn(1)
    send_own(1)

    for copy in small:
        copy.wait()
    codes = jnp.concatenate([codes_v[...], jnp.full((1, LANES), -1, jnp.int32)], axis=0)
    owner = (codes - HUBS) >> 5
    slot = (codes - HUBS) & 31

    def look(d, found):
        return jnp.where(owner == d, counts[d], found)

    filled = lax.fori_loop(0, RING * RING, look, jnp.zeros_like(codes), unroll=8)
    live = (codes >= 0) & ((codes < HUBS) | (slot < filled))
    codes = jnp.where(live, codes, -1)
    taken[...] = 1.0 + jnp.sum(live.astype(jnp.float32), axis=0, keepdims=True)
    req[...] = jnp.transpose(req_v[...])
    lane = lax.broadcasted_iota(jnp.int32, (RING, LANES), 1) // CAP
    for half in range(2):
        for place in range(RING):
            if half == 0:
                lists = req[place * RING : (place + 1) * RING]
            else:
                lists = req[pl.ds(place, RING, stride=RING)]
            lists = jnp.concatenate([lists] * 4, axis=1)
            meta_tx[half, place, 0:16] = codes
            meta_tx[half, place, 16:24] = jnp.where(lane == spot[half] % 4, lists, 0)
        meta_rx[half, spot[half], 0:16] = codes
    for half in range(2):
        meta_rx[half, spot[half], 16:24] = meta_tx[half, spot[half], 16:24]

    for hop in range(3):
        for way in range(2):
            for half in range(2):
                if hop < 2 or way == 0:
                    pl.semaphore_wait(token.at[half, way], 1)
                    if hop + way < 2:
                        tell(half, way)

    metas = []
    for step in (4, 3, 5, 2, 6, 1, 7):
        for half in range(2):
            place = (spot[half] + step) % RING
            copy = push(
                meta_tx.at[half, place], meta_rx.at[half, spot[half]],
                meta_send.at[half, step - 1], meta_recv.at[half, step - 1], cross[half](step),
            )
            launch(copy)
            metas.append(copy)
    for chunk in range(2, CHUNKS):
        turn(chunk)
        send_own(chunk)

    hub_sum = jnp.zeros((4 * LANES, LANES), jnp.float32)
    for chunk in range(CHUNKS):
        block = jnp.concatenate([ag[0, 0, chunk], ag[1, 0, chunk]], axis=0)
        rows = lax.broadcasted_iota(jnp.int32, (LANES, LANES), 0) + chunk * LANES
        pick = jnp.where(rows == hub_id[...], 1.0, 0.0).astype(jnp.bfloat16)
        hub_sum = hub_sum + dot(split(block), pick)
    hubs[0] = hub_sum[: 2 * LANES] + hub_sum[2 * LANES :]

    def hub_push(index, src, dst, peer):
        copy = push(src, dst, hub_send.at[index], hub_recv.at[index], peer)
        launch(copy)
        return copy

    hub_right = hub_push(0, hubs.at[0], hubs.at[2], along_x(1))
    hub_left = hub_push(1, hubs.at[0], hubs.at[6], along_x(XS - 1))
    hub_over = [hub_push(2, hubs.at[0], hubs.at[1], partner)]

    for copy in large:
        copy.wait()
    tot[...] = jnp.transpose(own[...])

    def relay(wave, chunk):
        for half in range(2):
            for way in range(2):
                moves[half, way, wave - 1, chunk].wait_recv()
                if wave < 3 or chunk // 2 == way:
                    moves[half, way, wave, chunk] = table(half, way, wave, chunk)
                    launch(moves[half, way, wave, chunk])

    relay(1, 0)
    relay(1, 1)
    for copy in metas:
        copy.wait_recv()
    for half in range(2):
        for group in range(2):
            tiles = [meta_rx[half, 4 * group + k, 16:24] for k in range(4)]
            ids[half, :, group * LANES : (group + 1) * LANES] = tiles[0] + tiles[1] + tiles[2] + tiles[3]

    def place_of(half, slot_index):
        mine = me[0] * (1 - half) + me[1] * half
        return (mine + RING - slot_index) % RING

    def pick_rows(half, slot_index, part_index):
        pieces = [ag[half, slot_index, 2 * part_index + k] for k in range(2)]
        block = split(jnp.concatenate(pieces, axis=1))
        wanted = ids[half, pl.ds(place_of(half, slot_index), 1), :]
        rows = lax.broadcasted_iota(jnp.int32, (2 * LANES, 2 * LANES), 0) + 2 * LANES * part_index
        return dot(block, jnp.where(rows == wanted, 1.0, 0.0).astype(jnp.bfloat16))

    def add_seeds(half, slot_index, rows):
        origin = place_of(half, slot_index)
        number = origin * (1 + half * (RING - 1)) + (me[1] * RING) * (1 - half) + me[0] * half
        lines = lax.broadcasted_iota(jnp.int32, (CAP, LANES), 0) + (HUBS + number * CAP)
        for place in range(RING):
            count = jnp.zeros((CAP, LANES), jnp.float32)
            for k in range(FAN):
                count = count + jnp.where(meta_rx[half, place, k : k + 1] == lines, 1.0, 0.0)
            top, left = CAP * (place % 4), LANES * (place % 2)
            cblk[place // 2, top : top + CAP, left : left + LANES] = count.astype(jnp.bfloat16)
        rows = rows.astype(jnp.bfloat16)
        for pair in range(RING // 2):
            side = (pair // 2) * LANES
            sums = dot(rows[:, side : side + LANES], cblk[pair])
            sums = sums[:LANES] + sums[LANES:]
            for k in range(2):
                pacc[half, 2 * pair + k] += sums[:, k * LANES : (k + 1) * LANES]

    def own_block(half, carry):
        add_seeds(half, 0, pick_rows(half, 0, 0) + pick_rows(half, 0, 1))
        return carry

    lax.fori_loop(0, 2, own_block, 0)

    def first_part(wave, index, carry):
        half, way = index // 2, index % 2
        slot_index = wave + way * (RING - 2 * wave)
        gacc[index] = pick_rows(half, slot_index, 0)
        return carry

    def second_part(wave, index, carry):
        half, way = index // 2, index % 2
        slot_index = wave + way * (RING - 2 * wave)
        add_seeds(half, slot_index, gacc[index] + pick_rows(half, slot_index, 1))
        return carry

    def hub_block(index, carry):
        chip, over = index // 2, index % 2
        origin = ((me_x + XS - chip) % XS) * 2 + (core + over) % 2
        lines = lax.broadcasted_iota(jnp.int32, (LANES, LANES), 0) + origin * LANES
        mine = spot[0]
        count = jnp.zeros((LANES, LANES), jnp.float32)
        for k in range(FAN):
            count = count + jnp.where(meta_rx[0, mine, k : k + 1] == lines, 1.0, 0.0)
        sums = dot(split(hubs[index]), count.astype(jnp.bfloat16))
        tot[...] += sums[: 2 * LANES] + sums[2 * LANES :]
        return carry

    for wave in range(1, 4):
        for chunk in range(CHUNKS):
            if wave > 1 or chunk > 1:
                relay(wave, chunk)
            if chunk == 1:
                lax.fori_loop(0, 4, functools.partial(first_part, wave), 0)
            if chunk == 3:
                lax.fori_loop(0, 4, functools.partial(second_part, wave), 0)
        if wave == 1:
            hub_right.wait_recv()
            hub_left.wait_recv()
            low, high = pl.ds(0, LANES), pl.ds(LANES, LANES)
            far = [
                hub_push(3, hubs.at[2, low], hubs.at[4, low], along_x(1)),
                hub_push(4, hubs.at[6, high], hubs.at[4, high], along_x(XS - 1)),
            ]
            hub_over.append(hub_push(5, hubs.at[2], hubs.at[3], partner))
            hub_over.append(hub_push(6, hubs.at[6], hubs.at[7], partner))
        if wave == 2:
            for copy in far:
                copy.wait_recv()
            hub_over.append(hub_push(7, hubs.at[4], hubs.at[5], partner))

    for copy in hub_over:
        copy.wait_recv()
    lax.fori_loop(0, 8, hub_block, 0)

    for chunk in (0, 2, 1, 3):
        for half in range(2):
            moves[half, chunk // 2, 3, chunk].wait_recv()

    sums_moves = []
    for half in range(2):
        add_seeds(half, 4, pick_rows(half, 4, 0) + pick_rows(half, 4, 1))
        for step in (4, 3, 5, 2, 6, 1, 7):
            copy = push(
                pacc.at[half, (spot[half] + step) % RING], part.at[half, step - 1],
                part_send.at[half, step - 1], part_recv.at[half, step - 1], cross[half](step),
            )
            launch(copy)
            sums_moves.append((half, step, copy))

    for half in range(2):
        tot[half * LANES : (half + 1) * LANES] += pacc[half, spot[half]]
    for wanted in (1, 7, 2, 6, 3, 5, 4):
        for half, step, copy in sums_moves:
            if step == wanted:
                copy.wait_recv()
                tot[half * LANES : (half + 1) * LANES] += part[half, step - 1]

    mean = jnp.transpose(tot[...] / taken[...])
    product = jnp.dot(mean, weight[...], precision=lax.Precision.HIGHEST, preferred_element_type=jnp.float32)
    out[...] = jnp.maximum(product + bias[...], 0.0)
    for copy in sent:
        copy.wait_send()


def local(features, seed_self, hub_ids, requests, counts, neighbors, weight, out_bias):
    hbm = pl.BlockSpec(memory_space=pltpu.HBM)
    vmem = pl.BlockSpec(memory_space=pltpu.VMEM)
    dma = pltpu.SemaphoreType.DMA
    return pl.pallas_call(
        kernel,
        out_shape=jax.ShapeDtypeStruct((SEEDS, 2 * LANES), jnp.float32),
        in_specs=[hbm] * 8,
        out_specs=vmem,
        scratch_shapes=[
            pltpu.VMEM((ROWS, 2 * LANES), jnp.float32),
            pltpu.VMEM((SEEDS, 2 * LANES), jnp.float32),
            pltpu.VMEM((1, LANES), jnp.int32),
            pltpu.VMEM((CAP, RING * RING), jnp.int32),
            pltpu.VMEM((RING * RING, CAP), jnp.int32),
            pltpu.SMEM((RING * RING,), jnp.int32),
            pltpu.VMEM((FAN, SEEDS), jnp.int32),
            pltpu.VMEM((2 * LANES, 2 * LANES), jnp.float32),
            pltpu.VMEM((1, 2 * LANES), jnp.float32),
            dma((11,)),
            pltpu.VMEM((2, RING, CHUNKS, LANES, LANES), jnp.float32),
            pltpu.VMEM((2, RING, 24, LANES), jnp.int32),
            pltpu.VMEM((2, RING, 24, LANES), jnp.int32),
            pltpu.VMEM((2, RING, 2 * LANES), jnp.int32),
            pltpu.VMEM((4, LANES, 2 * LANES), jnp.bfloat16),
            pltpu.VMEM((4, 2 * LANES, 2 * LANES), jnp.float32),
            pltpu.VMEM((2, RING, LANES, LANES), jnp.float32),
            pltpu.VMEM((2, RING - 1, LANES, LANES), jnp.float32),
            pltpu.VMEM((2 * XS, 2 * LANES, LANES), jnp.float32),
            pltpu.VMEM((2 * LANES, LANES), jnp.float32),
            pltpu.VMEM((1, LANES), jnp.float32),
            dma((2, 2, 4, CHUNKS)),
            dma((2, RING, CHUNKS)),
            dma((2, RING - 1)),
            dma((2, RING - 1)),
            dma((2, RING - 1)),
            dma((2, RING - 1)),
            dma((8,)),
            dma((8,)),
            pltpu.SemaphoreType.REGULAR((2, 2)),
        ],
        compiler_params=pltpu.CompilerParams(collective_id=0, has_side_effects=True),
        name="sage",
    )(features, seed_self, hub_ids.reshape(1, LANES), requests.T, counts, neighbors.T, weight, out_bias.reshape(1, 2 * LANES))


def solution(mesh):
    rows, flat = P(("rep", "shard"), None), P(("rep", "shard"))
    return jax.shard_map(
        local, mesh=mesh, in_specs=(rows, rows, flat, rows, flat, rows, P(), P()), out_specs=rows, check_vma=False
    )
```

```python
import functools

import jax
import jax.numpy as jnp
from jax import lax
from jax.experimental import pallas as pl
from jax.experimental.pallas import tpu as pltpu
from jax.sharding import PartitionSpec as P

MESH = pl.DeviceIdType.MESH
RING = 8
XS = 4
ROWS = 512
SEEDS = 128
FAN = 15
CAP = 32
HUBS = 1024
CHUNKS = 4
LANES = 128
WIDE = 64


def split(values):
    high = values.astype(jnp.bfloat16)
    low = (values - high.astype(jnp.float32)).astype(jnp.bfloat16)
    return jnp.concatenate([high, low], axis=0)


def dot(left, right):
    return jnp.dot(left, right, preferred_element_type=jnp.float32)


def kernel(
    feat_in, own_in, hub_in, req_in, counts_in, codes_in, weight_in, bias_in, out,
    feat, own, hub_id, req_v, req, counts, codes_v, weight, bias, fetch,
    ag, meta_tx, meta_rx, ids, cblk, pacc, part, hubs, tot, taken,
    ag_send, ag_recv, meta_send, meta_recv, part_send, part_recv, hub_send, hub_recv, token,
):
    rep = lax.axis_index("rep")
    shard = lax.axis_index("shard")
    me_x, core = rep // 2, rep % 2
    me = (shard % RING, shard // RING)

    def along_y(step):
        return {"rep": rep, "shard": me[1] * RING + (me[0] + step) % RING}

    def along_z(step):
        return {"rep": rep, "shard": ((me[1] + step) % RING) * RING + me[0]}

    def along_x(step):
        return {"rep": ((me_x + step) % XS) * 2 + core, "shard": shard}

    ring = (along_y, along_z)
    cross = (along_z, along_y)
    spot = (me[1], me[0])

    barrier = pltpu.get_barrier_semaphore()
    partner = {"rep": me_x * 2 + 1 - core, "shard": shard}
    peers = [along_y(1), along_y(RING - 1), along_z(1), along_z(RING - 1), along_x(1), along_x(XS - 1), partner]
    for peer in peers:
        pl.semaphore_signal(barrier, inc=1, device_id=peer, device_id_type=MESH)

    loads = []

    def load(src, dst):
        copy = pltpu.make_async_copy(src, dst, fetch.at[len(loads)])
        copy.start()
        loads.append(copy)
        return copy

    tables = [load(feat_in.at[pl.ds(c * LANES, LANES)], feat.at[pl.ds(c * LANES, LANES)]) for c in range(CHUNKS)]
    small = [load(codes_in, codes_v), load(counts_in, counts), load(req_in, req_v), load(hub_in, hub_id)]
    large = [load(own_in, own), load(weight_in, weight), load(bias_in, bias)]

    def push(src, dst, send, recv, peer):
        return pltpu.make_async_remote_copy(
            src_ref=src, dst_ref=dst, send_sem=send, recv_sem=recv, device_id=peer, device_id_type=MESH
        )

    sent = []

    def launch(copy):
        copy.start()
        sent.append(copy)
        return copy

    def table(half, way, wave, group, turn):
        piece = turn if way == 0 else 1 - turn
        slot_from = wave if way == 0 else (RING - wave) % RING
        slot_to = wave + 1 if way == 0 else RING - wave - 1
        return push(
            ag.at[half, slot_from, group, piece], ag.at[half, slot_to, group, piece],
            ag_send.at[half, way, wave, group, turn], ag_recv.at[half, slot_to, group, piece],
            ring[half](1 if way == 0 else RING - 1),
        )

    moves = {}

    def send_own(group):
        for turn in range(2):
            for half in range(2):
                for way in range(2):
                    moves[half, way, 0, group, turn] = launch(table(half, way, 0, group, turn))

    def tell(half, way):
        peer = ring[half](1 if way == 0 else RING - 1)
        pl.semaphore_signal(token.at[half, way], inc=1, device_id=peer, device_id_type=MESH)

    cblk[...] = jnp.zeros_like(cblk)
    for chunk in range(CHUNKS):
        tables[chunk].wait()
        for half in range(2):
            block = jnp.transpose(feat[chunk * LANES : (chunk + 1) * LANES, half * LANES : (half + 1) * LANES])
            left = (chunk % 2) * LANES
            for group in range(2):
                ag[half, 0, group, chunk // 2, :, left : left + LANES] = block[group * WIDE : (group + 1) * WIDE]
    pl.semaphore_wait(barrier, len(peers))
    for half in range(2):
        for way in range(2):
            tell(half, way)
    send_own(0)

    for copy in small:
        copy.wait()
    codes = jnp.concatenate([codes_v[...], jnp.full((1, LANES), -1, jnp.int32)], axis=0)
    owner = (codes - HUBS) >> 5
    slot = (codes - HUBS) & 31

    def look(d, found):
        return jnp.where(owner == d, counts[d], found)

    filled = lax.fori_loop(0, RING * RING, look, jnp.zeros_like(codes), unroll=8)
    live = (codes >= 0) & ((codes < HUBS) | (slot < filled))
    codes = jnp.where(live, codes, -1)
    taken[...] = 1.0 + jnp.sum(live.astype(jnp.float32), axis=0, keepdims=True)
    req[...] = jnp.transpose(req_v[...])
    lane = lax.broadcasted_iota(jnp.int32, (RING, LANES), 1) // CAP
    for half in range(2):
        for place in range(RING):
            if half == 0:
                lists = req[place * RING : (place + 1) * RING]
            else:
                lists = req[pl.ds(place, RING, stride=RING)]
            lists = jnp.concatenate([lists] * 4, axis=1)
            meta_tx[half, place, 0:16] = codes
            meta_tx[half, place, 16:24] = jnp.where(lane == spot[half] % 4, lists, 0)
        meta_rx[half, spot[half], 0:16] = codes
    for half in range(2):
        meta_rx[half, spot[half], 16:24] = meta_tx[half, spot[half], 16:24]

    for hop in range(3):
        for way in range(2):
            for half in range(2):
                if hop < 2 or way == 0:
                    pl.semaphore_wait(token.at[half, way], 1)
                    if hop + way < 2:
                        tell(half, way)

    metas = []
    for step in (4, 3, 5, 2, 6, 1, 7):
        for half in range(2):
            place = (spot[half] + step) % RING
            copy = push(
                meta_tx.at[half, place], meta_rx.at[half, spot[half]],
                meta_send.at[half, step - 1], meta_recv.at[half, step - 1], cross[half](step),
            )
            launch(copy)
            metas.append(copy)
    send_own(1)

    hub_sum = jnp.zeros((4 * LANES, LANES), jnp.float32)
    for piece in range(2):
        block = jnp.concatenate([ag[half, 0, group, piece] for half in range(2) for group in range(2)], axis=0)
        rows = lax.broadcasted_iota(jnp.int32, (2 * LANES, LANES), 0) + piece * 2 * LANES
        pick = jnp.where(rows == hub_id[...], 1.0, 0.0).astype(jnp.bfloat16)
        hub_sum = hub_sum + dot(split(block), pick)
    hubs[0] = hub_sum[: 2 * LANES] + hub_sum[2 * LANES :]

    def hub_push(index, src, dst, peer):
        copy = push(src, dst, hub_send.at[index], hub_recv.at[index], peer)
        launch(copy)
        return copy

    hub_right = hub_push(0, hubs.at[0], hubs.at[2], along_x(1))
    hub_left = hub_push(1, hubs.at[0], hubs.at[6], along_x(XS - 1))
    hub_over = [hub_push(2, hubs.at[0], hubs.at[1], partner)]

    for copy in large:
        copy.wait()
    tot[...] = jnp.transpose(own[...])

    def relay(wave, group, turn):
        for half in range(2):
            for way in range(2):
                moves[half, way, wave - 1, group, turn].wait_recv()
                if wave < 3 or turn == 0:
                    moves[half, way, wave, group, turn] = launch(table(half, way, wave, group, turn))

    def place_of(half, slot_index):
        return (me[half] + RING - slot_index) % RING

    def lay_counts(slots):
        for half in range(2):
            for slot_index in slots:
                origin = place_of(half, slot_index)
                number = me[1] * RING + origin if half == 0 else origin * RING + me[0]
                lines = lax.broadcasted_iota(jnp.int32, (CAP, LANES), 0) + (HUBS + number * CAP)
                for place in range(RING):
                    count = jnp.zeros((CAP, LANES), jnp.float32)
                    for k in range(FAN):
                        count = count + jnp.where(meta_rx[half, place, k : k + 1] == lines, 1.0, 0.0)
                    top, left = CAP * (place % 4), LANES * (place % 2)
                    cblk[half, slot_index, place // 2, top : top + CAP, left : left + LANES] = count.astype(jnp.bfloat16)

    def add_block(half, slot_index, group):
        block = jnp.concatenate([ag[half, slot_index, group, piece] for piece in range(2)], axis=1)
        wanted = ids[half, pl.ds(place_of(half, slot_index), 1), :]
        rows = lax.broadcasted_iota(jnp.int32, (ROWS, 2 * LANES), 0)
        found = dot(split(block), jnp.where(rows == wanted, 1.0, 0.0).astype(jnp.bfloat16)).astype(jnp.bfloat16)
        for pair in range(RING // 2):
            side = (pair // 2) * LANES
            sums = dot(found[:, side : side + LANES], cblk[half, slot_index, pair])
            sums = sums[:WIDE] + sums[WIDE:]
            for k in range(2):
                piece = sums[:, k * LANES : (k + 1) * LANES]
                if slot_index == 0:
                    pacc[half, 2 * pair + k, group] = piece
                else:
                    pacc[half, 2 * pair + k, group] += piece

    def add_blocks(slots, group):
        for slot_index in slots:
            for half in range(2):
                add_block(half, slot_index, group)

    def hub_block(index, carry):
        chip, over = index // 2, index % 2
        origin = ((me_x + XS - chip) % XS) * 2 + (core + over) % 2
        lines = lax.broadcasted_iota(jnp.int32, (LANES, LANES), 0) + origin * LANES
        mine = spot[0]
        count = jnp.zeros((LANES, LANES), jnp.float32)
        for k in range(FAN):
            count = count + jnp.where(meta_rx[0, mine, k : k + 1] == lines, 1.0, 0.0)
        sums = dot(split(hubs[index]), count.astype(jnp.bfloat16))
        tot[...] += sums[: 2 * LANES] + sums[2 * LANES :]
        return carry

    relay(1, 0, 0)
    relay(1, 0, 1)
    for copy in metas:
        copy.wait_recv()
    for half in range(2):
        for group in range(2):
            tiles = [meta_rx[half, 4 * group + k, 16:24] for k in range(4)]
            ids[half, :, group * LANES : (group + 1) * LANES] = tiles[0] + tiles[1] + tiles[2] + tiles[3]
    lay_counts((0,))
    add_blocks((0,), 0)
    add_blocks((0,), 1)
    relay(1, 1, 0)
    relay(1, 1, 1)
    hub_right.wait_recv()
    hub_left.wait_recv()
    low, high = pl.ds(0, LANES), pl.ds(LANES, LANES)
    far = [
        hub_push(3, hubs.at[2, low], hubs.at[4, low], along_x(1)),
        hub_push(4, hubs.at[6, high], hubs.at[4, high], along_x(XS - 1)),
    ]
    hub_over.append(hub_push(5, hubs.at[2], hubs.at[3], partner))
    hub_over.append(hub_push(6, hubs.at[6], hubs.at[7], partner))
    lay_counts((1, 7))
    add_blocks((1, 7), 0)
    relay(2, 0, 0)
    relay(2, 0, 1)
    for copy in far:
        copy.wait_recv()
    hub_over.append(hub_push(7, hubs.at[4], hubs.at[5], partner))
    add_blocks((1, 7), 1)
    lay_counts((2, 6))
    relay(2, 1, 0)
    add_blocks((2, 6), 0)
    relay(3, 0, 0)
    lay_counts((3, 5))
    relay(2, 1, 1)
    relay(3, 0, 1)
    add_blocks((3, 5), 0)
    lay_counts((4,))
    relay(3, 1, 0)
    add_blocks((2, 6), 1)

    sums_moves = []

    def finish(group):
        for half in range(2):
            for way in range(2):
                moves[half, way, 3, group, 0].wait_recv()
        for half in range(2):
            add_block(half, 4, group)
            for step in (4, 3, 5, 2, 6, 1, 7):
                copy = push(
                    pacc.at[half, (spot[half] + step) % RING, group], part.at[half, step - 1, group],
                    part_send.at[half, group, step - 1], part_recv.at[half, group, step - 1], cross[half](step),
                )
                launch(copy)
                sums_moves.append((half, step, group, copy))

    finish(0)
    relay(3, 1, 1)
    add_blocks((3, 5), 1)
    finish(1)
    for copy in hub_over:
        copy.wait_recv()
    lax.fori_loop(0, 8, hub_block, 0, unroll=True)

    product = jnp.zeros((SEEDS, 2 * LANES), jnp.float32)
    for group in range(2):
        lines = []
        for half in range(2):
            top = half * LANES + group * WIDE
            total = tot[top : top + WIDE] + pacc[half, spot[half], group]
            for wanted in (1, 7, 2, 6, 3, 5, 4):
                for side, step, number, copy in sums_moves:
                    if (side, step, number) == (half, wanted, group):
                        copy.wait_recv()
                        total = total + part[half, step - 1, group]
            lines.append(total)
        mean = jnp.transpose(jnp.concatenate(lines, axis=0) / taken[...])
        parts = [weight[half * LANES + group * WIDE : half * LANES + (group + 1) * WIDE] for half in range(2)]
        product = product + jnp.dot(
            mean, jnp.concatenate(parts, axis=0), precision=lax.Precision.HIGHEST, preferred_element_type=jnp.float32
        )
    out[...] = jnp.maximum(product + bias[...], 0.0)
    for copy in sent:
        copy.wait_send()


def local(features, seed_self, hub_ids, requests, counts, neighbors, weight, out_bias):
    hbm = pl.BlockSpec(memory_space=pltpu.HBM)
    vmem = pl.BlockSpec(memory_space=pltpu.VMEM)
    dma = pltpu.SemaphoreType.DMA
    return pl.pallas_call(
        kernel,
        out_shape=jax.ShapeDtypeStruct((SEEDS, 2 * LANES), jnp.float32),
        in_specs=[hbm] * 8,
        out_specs=vmem,
        scratch_shapes=[
            pltpu.VMEM((ROWS, 2 * LANES), jnp.float32),
            pltpu.VMEM((SEEDS, 2 * LANES), jnp.float32),
            pltpu.VMEM((1, LANES), jnp.int32),
            pltpu.VMEM((CAP, RING * RING), jnp.int32),
            pltpu.VMEM((RING * RING, CAP), jnp.int32),
            pltpu.SMEM((RING * RING,), jnp.int32),
            pltpu.VMEM((FAN, SEEDS), jnp.int32),
            pltpu.VMEM((2 * LANES, 2 * LANES), jnp.float32),
            pltpu.VMEM((1, 2 * LANES), jnp.float32),
            dma((11,)),
            pltpu.VMEM((2, RING, 2, 2, WIDE, 2 * LANES), jnp.float32),
            pltpu.VMEM((2, RING, 24, LANES), jnp.int32),
            pltpu.VMEM((2, RING, 24, LANES), jnp.int32),
            pltpu.VMEM((2, RING, 2 * LANES), jnp.int32),
            pltpu.VMEM((2, RING, 4, LANES, 2 * LANES), jnp.bfloat16),
            pltpu.VMEM((2, RING, 2, WIDE, LANES), jnp.float32),
            pltpu.VMEM((2, RING - 1, 2, WIDE, LANES), jnp.float32),
            pltpu.VMEM((2 * XS, 2 * LANES, LANES), jnp.float32),
            pltpu.VMEM((2 * LANES, LANES), jnp.float32),
            pltpu.VMEM((1, LANES), jnp.float32),
            dma((2, 2, 4, 2, 2)),
            dma((2, RING, 2, 2)),
            dma((2, RING - 1)),
            dma((2, RING - 1)),
            dma((2, 2, RING - 1)),
            dma((2, 2, RING - 1)),
            dma((8,)),
            dma((8,)),
            pltpu.SemaphoreType.REGULAR((2, 2)),
        ],
        compiler_params=pltpu.CompilerParams(collective_id=0, has_side_effects=True),
        name="sage",
    )(features, seed_self, hub_ids.reshape(1, LANES), requests.T, counts, neighbors.T, weight, out_bias.reshape(1, 2 * LANES))


def solution(mesh):
    rows, flat = P(("rep", "shard"), None), P(("rep", "shard"))
    return jax.shard_map(
        local, mesh=mesh, in_specs=(rows, rows, flat, rows, flat, rows, P(), P()), out_specs=rows, check_vma=False
    )
```

```python
import functools

import jax
import jax.numpy as jnp
from jax import lax
from jax.experimental import pallas as pl
from jax.experimental.pallas import tpu as pltpu
from jax.sharding import PartitionSpec as P

MESH = pl.DeviceIdType.MESH
RING = 8
XS = 4
ROWS = 512
SEEDS = 128
FAN = 15
CAP = 32
HUBS = 1024
CHUNKS = 4
LANES = 128
WIDE = 64


def split(values):
    high = values.astype(jnp.bfloat16)
    low = (values - high.astype(jnp.float32)).astype(jnp.bfloat16)
    return jnp.concatenate([high, low], axis=0)


def dot(left, right):
    return jnp.dot(left, right, preferred_element_type=jnp.float32)


def kernel(
    feat_in, own_in, hub_in, req_in, counts_in, codes_in, weight_in, bias_in, out,
    feat, own, hub_id, req_v, req, counts, codes_v, weight, bias, fetch,
    ag, meta_tx, meta_rx, ids, cblk, pacc, part, hubs, tot, taken,
    ag_send, ag_recv, meta_send, meta_recv, part_send, part_recv, hub_send, hub_recv, token,
):
    rep = lax.axis_index("rep")
    shard = lax.axis_index("shard")
    me_x, core = rep // 2, rep % 2
    me = (shard % RING, shard // RING)

    def along_y(step):
        return {"rep": rep, "shard": me[1] * RING + (me[0] + step) % RING}

    def along_z(step):
        return {"rep": rep, "shard": ((me[1] + step) % RING) * RING + me[0]}

    def along_x(step):
        return {"rep": ((me_x + step) % XS) * 2 + core, "shard": shard}

    ring = (along_y, along_z)
    cross = (along_z, along_y)
    spot = (me[1], me[0])

    barrier = pltpu.get_barrier_semaphore()
    partner = {"rep": me_x * 2 + 1 - core, "shard": shard}
    peers = [along_y(1), along_y(RING - 1), along_z(1), along_z(RING - 1), along_x(1), along_x(XS - 1), partner]
    for peer in peers:
        pl.semaphore_signal(barrier, inc=1, device_id=peer, device_id_type=MESH)

    loads = []

    def load(src, dst):
        copy = pltpu.make_async_copy(src, dst, fetch.at[len(loads)])
        copy.start()
        loads.append(copy)
        return copy

    tables = [load(feat_in.at[pl.ds(c * LANES, LANES)], feat.at[pl.ds(c * LANES, LANES)]) for c in range(CHUNKS)]
    small = [load(codes_in, codes_v), load(counts_in, counts), load(req_in, req_v), load(hub_in, hub_id)]
    large = [load(own_in, own), load(weight_in, weight), load(bias_in, bias)]

    def push(src, dst, send, recv, peer):
        return pltpu.make_async_remote_copy(
            src_ref=src, dst_ref=dst, send_sem=send, recv_sem=recv, device_id=peer, device_id_type=MESH
        )

    sent = []

    def launch(copy):
        copy.start()
        sent.append(copy)
        return copy

    def table(half, way, wave, group, turn):
        piece = turn if way == 0 else 1 - turn
        slot_from = wave if way == 0 else (RING - wave) % RING
        slot_to = wave + 1 if way == 0 else RING - wave - 1
        return push(
            ag.at[half, slot_from, group, piece], ag.at[half, slot_to, group, piece],
            ag_send.at[half, way, wave, group, turn], ag_recv.at[half, slot_to, group, piece],
            ring[half](1 if way == 0 else RING - 1),
        )

    moves = {}

    def send_own(group):
        for turn in range(2):
            for half in range(2):
                for way in range(2):
                    moves[half, way, 0, group, turn] = launch(table(half, way, 0, group, turn))

    def tell(half, way):
        peer = ring[half](1 if way == 0 else RING - 1)
        pl.semaphore_signal(token.at[half, way], inc=1, device_id=peer, device_id_type=MESH)

    cblk[...] = jnp.zeros_like(cblk)
    for chunk in range(CHUNKS):
        tables[chunk].wait()
        for half in range(2):
            block = jnp.transpose(feat[chunk * LANES : (chunk + 1) * LANES, half * LANES : (half + 1) * LANES])
            left = (chunk % 2) * LANES
            for group in range(2):
                ag[half, 0, group, chunk // 2, :, left : left + LANES] = block[group * WIDE : (group + 1) * WIDE]
    pl.semaphore_wait(barrier, len(peers))
    for half in range(2):
        for way in range(2):
            tell(half, way)
    send_own(0)

    for copy in small:
        copy.wait()
    codes = jnp.concatenate([codes_v[...], jnp.full((1, LANES), -1, jnp.int32)], axis=0)
    owner = (codes - HUBS) >> 5
    slot = (codes - HUBS) & 31

    def look(d, found):
        return jnp.where(owner == d, counts[d], found)

    filled = lax.fori_loop(0, RING * RING, look, jnp.zeros_like(codes), unroll=8)
    live = (codes >= 0) & ((codes < HUBS) | (slot < filled))
    codes = jnp.where(live, codes, -1)
    taken[...] = 1.0 + jnp.sum(live.astype(jnp.float32), axis=0, keepdims=True)
    req[...] = jnp.transpose(req_v[...])
    lane = lax.broadcasted_iota(jnp.int32, (RING, LANES), 1) // CAP
    for half in range(2):
        for place in range(RING):
            if half == 0:
                lists = req[place * RING : (place + 1) * RING]
            else:
                lists = req[pl.ds(place, RING, stride=RING)]
            lists = jnp.concatenate([lists] * 4, axis=1)
            meta_tx[half, place, 0:16] = codes
            meta_tx[half, place, 16:24] = jnp.where(lane == spot[half] % 4, lists, 0)
        meta_rx[half, spot[half], 0:16] = codes
    for half in range(2):
        meta_rx[half, spot[half], 16:24] = meta_tx[half, spot[half], 16:24]

    for hop in range(3):
        for way in range(2):
            for half in range(2):
                if hop < 2 or way == 0:
                    pl.semaphore_wait(token.at[half, way], 1)
                    if hop + way < 2:
                        tell(half, way)

    metas = []
    for step in (4, 3, 5, 2, 6, 1, 7):
        for half in range(2):
            place = (spot[half] + step) % RING
            copy = push(
                meta_tx.at[half, place], meta_rx.at[half, spot[half]],
                meta_send.at[half, step - 1], meta_recv.at[half, step - 1], cross[half](step),
            )
            launch(copy)
            metas.append(copy)
    send_own(1)

    hub_sum = jnp.zeros((4 * LANES, LANES), jnp.float32)
    for piece in range(2):
        block = jnp.concatenate([ag[half, 0, group, piece] for half in range(2) for group in range(2)], axis=0)
        rows = lax.broadcasted_iota(jnp.int32, (2 * LANES, LANES), 0) + piece * 2 * LANES
        pick = jnp.where(rows == hub_id[...], 1.0, 0.0).astype(jnp.bfloat16)
        hub_sum = hub_sum + dot(split(block), pick)
    hubs[0] = hub_sum[: 2 * LANES] + hub_sum[2 * LANES :]

    def hub_push(index, src, dst, peer):
        copy = push(src, dst, hub_send.at[index], hub_recv.at[index], peer)
        launch(copy)
        return copy

    hub_right = hub_push(0, hubs.at[0], hubs.at[2], along_x(1))
    hub_left = hub_push(1, hubs.at[0], hubs.at[6], along_x(XS - 1))
    hub_over = [hub_push(2, hubs.at[0], hubs.at[1], partner)]

    for copy in large:
        copy.wait()
    tot[...] = jnp.transpose(own[...])

    def relay(wave, group, turn):
        for half in range(2):
            for way in range(2):
                moves[half, way, wave - 1, group, turn].wait_recv()
                if wave < 3 or turn == 0:
                    moves[half, way, wave, group, turn] = launch(table(half, way, wave, group, turn))

    def place_of(half, slot_index):
        return (me[half] + RING - slot_index) % RING

    def lay_counts(slots):
        for half in range(2):
            for slot_index in slots:
                origin = place_of(half, slot_index)
                number = me[1] * RING + origin if half == 0 else origin * RING + me[0]
                lines = lax.broadcasted_iota(jnp.int32, (CAP, LANES), 0) + (HUBS + number * CAP)
                for place in range(RING):
                    count = jnp.zeros((CAP, LANES), jnp.float32)
                    for k in range(FAN):
                        count = count + jnp.where(meta_rx[half, place, k : k + 1] == lines, 1.0, 0.0)
                    top, left = CAP * (place % 4), LANES * (place % 2)
                    cblk[half, slot_index, place // 2, top : top + CAP, left : left + LANES] = count.astype(jnp.bfloat16)

    def add_block(half, slot_index, group):
        block = jnp.concatenate([ag[half, slot_index, group, piece] for piece in range(2)], axis=1)
        wanted = ids[half, pl.ds(place_of(half, slot_index), 1), :]
        rows = lax.broadcasted_iota(jnp.int32, (ROWS, 2 * LANES), 0)
        found = dot(split(block), jnp.where(rows == wanted, 1.0, 0.0).astype(jnp.bfloat16)).astype(jnp.bfloat16)
        for pair in range(RING // 2):
            side = (pair // 2) * LANES
            sums = dot(found[:, side : side + LANES], cblk[half, slot_index, pair])
            sums = sums[:WIDE] + sums[WIDE:]
            for k in range(2):
                piece = sums[:, k * LANES : (k + 1) * LANES]
                if slot_index == 0:
                    pacc[half, 2 * pair + k, group] = piece
                else:
                    pacc[half, 2 * pair + k, group] += piece

    def add_blocks(slots, group):
        for slot_index in slots:
            for half in range(2):
                add_block(half, slot_index, group)

    def hub_block(index, carry):
        chip, over = index // 2, index % 2
        origin = ((me_x + XS - chip) % XS) * 2 + (core + over) % 2
        lines = lax.broadcasted_iota(jnp.int32, (LANES, LANES), 0) + origin * LANES
        mine = spot[0]
        count = jnp.zeros((LANES, LANES), jnp.float32)
        for k in range(FAN):
            count = count + jnp.where(meta_rx[0, mine, k : k + 1] == lines, 1.0, 0.0)
        sums = dot(split(hubs[index]), count.astype(jnp.bfloat16))
        tot[...] += sums[: 2 * LANES] + sums[2 * LANES :]
        return carry

    relay(1, 0, 0)
    relay(1, 0, 1)
    for copy in metas:
        copy.wait_recv()
    for half in range(2):
        for group in range(2):
            tiles = [meta_rx[half, 4 * group + k, 16:24] for k in range(4)]
            ids[half, :, group * LANES : (group + 1) * LANES] = tiles[0] + tiles[1] + tiles[2] + tiles[3]
    lay_counts((0,))
    add_blocks((0,), 0)
    add_blocks((0,), 1)
    relay(1, 1, 0)
    relay(1, 1, 1)
    hub_right.wait_recv()
    hub_left.wait_recv()
    low, high = pl.ds(0, LANES), pl.ds(LANES, LANES)
    far = [
        hub_push(3, hubs.at[2, low], hubs.at[4, low], along_x(1)),
        hub_push(4, hubs.at[6, high], hubs.at[4, high], along_x(XS - 1)),
    ]
    hub_over.append(hub_push(5, hubs.at[2], hubs.at[3], partner))
    hub_over.append(hub_push(6, hubs.at[6], hubs.at[7], partner))
    lay_counts((1, 7))
    add_blocks((1, 7), 0)
    relay(2, 0, 0)
    relay(2, 0, 1)
    for copy in far:
        copy.wait_recv()
    hub_over.append(hub_push(7, hubs.at[4], hubs.at[5], partner))
    add_blocks((1, 7), 1)
    lay_counts((2, 6))
    relay(2, 1, 0)
    add_blocks((2, 6), 0)
    relay(3, 0, 0)
    lay_counts((3, 5))
    relay(2, 1, 1)
    relay(3, 0, 1)
    add_blocks((3, 5), 0)
    lay_counts((4,))
    relay(3, 1, 0)
    add_blocks((2, 6), 1)

    sums_moves = []

    def finish(group):
        for half in range(2):
            for way in range(2):
                moves[half, way, 3, group, 0].wait_recv()
        for half in range(2):
            add_block(half, 4, group)
            for step in (4, 3, 5, 2, 6, 1, 7):
                copy = push(
                    pacc.at[half, (spot[half] + step) % RING, group], part.at[half, step - 1, group],
                    part_send.at[half, group, step - 1], part_recv.at[half, group, step - 1], cross[half](step),
                )
                launch(copy)
                sums_moves.append((half, step, group, copy))

    finish(0)
    relay(3, 1, 1)
    add_blocks((3, 5), 1)
    finish(1)
    for copy in hub_over:
        copy.wait_recv()
    lax.fori_loop(0, 8, hub_block, 0, unroll=True)

    product = jnp.zeros((SEEDS, 2 * LANES), jnp.float32)
    for group in range(2):
        lines = []
        for half in range(2):
            top = half * LANES + group * WIDE
            total = tot[top : top + WIDE] + pacc[half, spot[half], group]
            for wanted in (1, 7, 2, 6, 3, 5, 4):
                for side, step, number, copy in sums_moves:
                    if (side, step, number) == (half, wanted, group):
                        copy.wait_recv()
                        total = total + part[half, step - 1, group]
            lines.append(total)
        mean = jnp.transpose(jnp.concatenate(lines, axis=0) / taken[...])
        parts = [weight[half * LANES + group * WIDE : half * LANES + (group + 1) * WIDE] for half in range(2)]
        product = product + jnp.dot(
            mean, jnp.concatenate(parts, axis=0), precision=lax.Precision.HIGHEST, preferred_element_type=jnp.float32
        )
    out[...] = jnp.maximum(product + bias[...], 0.0)
    for copy in sent:
        copy.wait_send()


def local(features, seed_self, hub_ids, requests, counts, neighbors, weight, out_bias):
    hbm = pl.BlockSpec(memory_space=pltpu.HBM)
    vmem = pl.BlockSpec(memory_space=pltpu.VMEM)
    dma = pltpu.SemaphoreType.DMA
    return pl.pallas_call(
        kernel,
        out_shape=jax.ShapeDtypeStruct((SEEDS, 2 * LANES), jnp.float32),
        in_specs=[hbm] * 8,
        out_specs=vmem,
        scratch_shapes=[
            pltpu.VMEM((ROWS, 2 * LANES), jnp.float32),
            pltpu.VMEM((SEEDS, 2 * LANES), jnp.float32),
            pltpu.VMEM((1, LANES), jnp.int32),
            pltpu.VMEM((CAP, RING * RING), jnp.int32),
            pltpu.VMEM((RING * RING, CAP), jnp.int32),
            pltpu.SMEM((RING * RING,), jnp.int32),
            pltpu.VMEM((FAN, SEEDS), jnp.int32),
            pltpu.VMEM((2 * LANES, 2 * LANES), jnp.float32),
            pltpu.VMEM((1, 2 * LANES), jnp.float32),
            dma((11,)),
            pltpu.VMEM((2, RING, 2, 2, WIDE, 2 * LANES), jnp.float32),
            pltpu.VMEM((2, RING, 24, LANES), jnp.int32),
            pltpu.VMEM((2, RING, 24, LANES), jnp.int32),
            pltpu.VMEM((2, RING, 2 * LANES), jnp.int32),
            pltpu.VMEM((2, RING, 4, LANES, 2 * LANES), jnp.bfloat16),
            pltpu.VMEM((2, RING, 2, WIDE, LANES), jnp.float32),
            pltpu.VMEM((2, RING - 1, 2, WIDE, LANES), jnp.float32),
            pltpu.VMEM((2 * XS, 2 * LANES, LANES), jnp.float32),
            pltpu.VMEM((2 * LANES, LANES), jnp.float32),
            pltpu.VMEM((1, LANES), jnp.float32),
            dma((2, 2, 4, 2, 2)),
            dma((2, RING, 2, 2)),
            dma((2, RING - 1)),
            dma((2, RING - 1)),
            dma((2, 2, RING - 1)),
            dma((2, 2, RING - 1)),
            dma((8,)),
            dma((8,)),
            pltpu.SemaphoreType.REGULAR((2, 2)),
        ],
        compiler_params=pltpu.CompilerParams(collective_id=0, has_side_effects=True, vmem_limit_bytes=40 * 1024 * 1024),
        name="sage",
    )(
        *(
            pltpu.with_memory_space_constraint(x, pltpu.HBM)
            for x in (
                features, seed_self, hub_ids.reshape(1, LANES), requests.T, counts, neighbors.T, weight,
                out_bias.reshape(1, 2 * LANES),
            )
        )
    )


def solution(mesh):
    rows, flat = P(("rep", "shard"), None), P(("rep", "shard"))
    return jax.shard_map(
        local, mesh=mesh, in_specs=(rows, rows, flat, rows, flat, rows, P(), P()), out_specs=rows, check_vma=False
    )
```

```python
import functools

import jax
import jax.numpy as jnp
from jax import lax
from jax.experimental import pallas as pl
from jax.experimental.pallas import tpu as pltpu
from jax.sharding import PartitionSpec as P

MESH = pl.DeviceIdType.MESH
RING = 8
XS = 4
ROWS = 512
SEEDS = 128
FAN = 15
CAP = 32
HUBS = 1024
CHUNKS = 4
LANES = 128
WIDE = 64


def split(values):
    high = values.astype(jnp.bfloat16)
    low = (values - high.astype(jnp.float32)).astype(jnp.bfloat16)
    return jnp.concatenate([high, low], axis=0)


def dot(left, right):
    return jnp.dot(left, right, preferred_element_type=jnp.float32)


def kernel(
    feat_in, own_in, hub_in, req_in, counts_in, codes_in, weight_in, bias_in, out,
    feat, own, hub_id, req_v, req, counts, codes_v, weight, bias, fetch,
    ag, meta_tx, meta_rx, ids, cblk, pacc, part, hubs, tot, taken,
    send, recv, ag_recv, token,
):
    rep = lax.axis_index("rep")
    shard = lax.axis_index("shard")
    me_x, core = rep // 2, rep % 2
    me = (shard % RING, shard // RING)

    def along_y(step):
        return {"rep": rep, "shard": me[1] * RING + (me[0] + step) % RING}

    def along_z(step):
        return {"rep": rep, "shard": ((me[1] + step) % RING) * RING + me[0]}

    def along_x(step):
        return {"rep": ((me_x + step) % XS) * 2 + core, "shard": shard}

    ring = (along_y, along_z)
    cross = (along_z, along_y)
    spot = (me[1], me[0])

    barrier = pltpu.get_barrier_semaphore()
    partner = {"rep": me_x * 2 + 1 - core, "shard": shard}
    peers = [along_y(1), along_y(RING - 1), along_z(1), along_z(RING - 1), along_x(1), along_x(XS - 1), partner]
    for peer in peers:
        pl.semaphore_signal(barrier, inc=1, device_id=peer, device_id_type=MESH)

    loads = []

    def load(src, dst):
        copy = pltpu.make_async_copy(src, dst, fetch.at[len(loads)])
        copy.start()
        loads.append(copy)
        return copy

    tables = load(feat_in, feat)
    small = [load(codes_in, codes_v), load(counts_in, counts), load(req_in, req_v), load(hub_in, hub_id)]
    large = [load(own_in, own), load(weight_in, weight), load(bias_in, bias)]

    def push(src, dst, send, recv, peer):
        return pltpu.make_async_remote_copy(
            src_ref=src, dst_ref=dst, send_sem=send, recv_sem=recv, device_id=peer, device_id_type=MESH
        )

    def launch(copy):
        copy.start()
        return copy

    def drain(semaphore, view):
        pltpu.make_async_copy(view, view, semaphore).wait()

    def table(half, way, wave, group, turn):
        piece = turn if way == 0 else 1 - turn
        slot_from = wave if way == 0 else (RING - wave) % RING
        slot_to = wave + 1 if way == 0 else RING - wave - 1
        return push(
            ag.at[half, slot_from, group, piece], ag.at[half, slot_to, group, piece],
            send.at[0], ag_recv.at[half, wave, group, turn],
            ring[half](1 if way == 0 else RING - 1),
        )

    def send_own(group):
        for turn in range(2):
            for half in range(2):
                for way in range(2):
                    launch(table(half, way, 0, group, turn))

    def tell(half, way):
        peer = ring[half](1 if way == 0 else RING - 1)
        pl.semaphore_signal(token.at[half, way], inc=1, device_id=peer, device_id_type=MESH)

    cblk[...] = jnp.zeros_like(cblk)
    tables.wait()
    for chunk in range(CHUNKS):
        for half in range(2):
            block = jnp.transpose(feat[chunk * LANES : (chunk + 1) * LANES, half * LANES : (half + 1) * LANES])
            left = (chunk % 2) * LANES
            for group in range(2):
                ag[half, 0, group, chunk // 2, :, left : left + LANES] = block[group * WIDE : (group + 1) * WIDE]
    pl.semaphore_wait(barrier, len(peers))
    for half in range(2):
        for way in range(2):
            tell(half, way)
    send_own(0)

    for copy in small:
        copy.wait()
    codes = jnp.concatenate([codes_v[...], jnp.full((1, LANES), -1, jnp.int32)], axis=0)
    owner = (codes - HUBS) >> 5
    slot = (codes - HUBS) & 31

    def look(d, found):
        return jnp.where(owner == d, counts[d], found)

    filled = lax.fori_loop(0, RING * RING, look, jnp.zeros_like(codes), unroll=8)
    live = (codes >= 0) & ((codes < HUBS) | (slot < filled))
    codes = jnp.where(live, codes, -1)
    taken[...] = 1.0 + jnp.sum(live.astype(jnp.float32), axis=0, keepdims=True)
    req[...] = jnp.transpose(req_v[...])
    lane = lax.broadcasted_iota(jnp.int32, (RING, LANES), 1) // CAP
    for half in range(2):
        for place in range(RING):
            if half == 0:
                lists = req[place * RING : (place + 1) * RING]
            else:
                lists = req[pl.ds(place, RING, stride=RING)]
            lists = jnp.concatenate([lists] * 4, axis=1)
            meta_tx[half, place, 0:16] = codes
            meta_tx[half, place, 16:24] = jnp.where(lane == spot[half] % 4, lists, 0)
        meta_rx[half, spot[half], 0:16] = codes
    for half in range(2):
        meta_rx[half, spot[half], 16:24] = meta_tx[half, spot[half], 16:24]

    for hop in range(3):
        for way in range(2):
            for half in range(2):
                if hop < 2 or way == 0:
                    pl.semaphore_wait(token.at[half, way], 1)
                    if hop + way < 2:
                        tell(half, way)

    for step in (4, 3, 5, 2, 6, 1, 7):
        for half in range(2):
            place = (spot[half] + step) % RING
            copy = push(
                meta_tx.at[half, place], meta_rx.at[half, spot[half]],
                send.at[1], recv.at[0], cross[half](step),
            )
            launch(copy)
    send_own(1)

    hub_sum = jnp.zeros((4 * LANES, LANES), jnp.float32)
    for piece in range(2):
        block = jnp.concatenate([ag[half, 0, group, piece] for half in range(2) for group in range(2)], axis=0)
        rows = lax.broadcasted_iota(jnp.int32, (2 * LANES, LANES), 0) + piece * 2 * LANES
        pick = jnp.where(rows == hub_id[...], 1.0, 0.0).astype(jnp.bfloat16)
        hub_sum = hub_sum + dot(split(block), pick)
    hubs[0] = hub_sum[: 2 * LANES] + hub_sum[2 * LANES :]

    def hub_push(index, src, dst, peer):
        launch(push(src, dst, send.at[2], recv.at[index], peer))

    hub_push(1, hubs.at[0], hubs.at[2], along_x(1))
    hub_push(1, hubs.at[0], hubs.at[6], along_x(XS - 1))
    hub_push(3, hubs.at[0], hubs.at[1], partner)

    for copy in large:
        copy.wait()
    tot[...] = jnp.transpose(own[...])

    def relay(wave, group, turn):
        for half in range(2):
            drain(ag_recv.at[half, wave - 1, group, turn], ag.at[half, 0, 0])
            if wave < 3 or turn == 0:
                for way in range(2):
                    launch(table(half, way, wave, group, turn))

    def place_of(half, slot_index):
        return (me[half] + RING - slot_index) % RING

    def lay_counts(slots):
        for half in range(2):
            for slot_index in slots:
                origin = place_of(half, slot_index)
                number = me[1] * RING + origin if half == 0 else origin * RING + me[0]
                lines = lax.broadcasted_iota(jnp.int32, (CAP, LANES), 0) + (HUBS + number * CAP)
                for place in range(RING):
                    count = jnp.zeros((CAP, LANES), jnp.float32)
                    for k in range(FAN):
                        count = count + jnp.where(meta_rx[half, place, k : k + 1] == lines, 1.0, 0.0)
                    top, left = CAP * (place % 4), LANES * (place % 2)
                    cblk[half, slot_index, place // 2, top : top + CAP, left : left + LANES] = count.astype(jnp.bfloat16)

    def add_block(half, slot_index, group):
        block = jnp.concatenate([ag[half, slot_index, group, piece] for piece in range(2)], axis=1)
        wanted = ids[half, pl.ds(place_of(half, slot_index), 1), :]
        rows = lax.broadcasted_iota(jnp.int32, (ROWS, 2 * LANES), 0)
        found = dot(split(block), jnp.where(rows == wanted, 1.0, 0.0).astype(jnp.bfloat16)).astype(jnp.bfloat16)
        for pair in range(RING // 2):
            side = (pair // 2) * LANES
            sums = dot(found[:, side : side + LANES], cblk[half, slot_index, pair])
            sums = sums[:WIDE] + sums[WIDE:]
            for k in range(2):
                piece = sums[:, k * LANES : (k + 1) * LANES]
                if slot_index == 0:
                    pacc[half, 2 * pair + k, group] = piece
                else:
                    pacc[half, 2 * pair + k, group] += piece

    def add_blocks(slots, group):
        for slot_index in slots:
            for half in range(2):
                add_block(half, slot_index, group)

    def hub_block(index, carry):
        chip, over = index // 2, index % 2
        origin = ((me_x + XS - chip) % XS) * 2 + (core + over) % 2
        lines = lax.broadcasted_iota(jnp.int32, (LANES, LANES), 0) + origin * LANES
        mine = spot[0]
        count = jnp.zeros((LANES, LANES), jnp.float32)
        for k in range(FAN):
            count = count + jnp.where(meta_rx[0, mine, k : k + 1] == lines, 1.0, 0.0)
        sums = dot(split(hubs[index]), count.astype(jnp.bfloat16))
        tot[...] += sums[: 2 * LANES] + sums[2 * LANES :]
        return carry

    relay(1, 0, 0)
    relay(1, 0, 1)
    drain(recv.at[0], meta_rx.at[:, pl.ds(0, RING - 1)])
    for half in range(2):
        for group in range(2):
            tiles = [meta_rx[half, 4 * group + k, 16:24] for k in range(4)]
            ids[half, :, group * LANES : (group + 1) * LANES] = tiles[0] + tiles[1] + tiles[2] + tiles[3]
    lay_counts((0,))
    add_blocks((0,), 0)
    add_blocks((0,), 1)
    relay(1, 1, 0)
    relay(1, 1, 1)
    drain(recv.at[1], hubs.at[pl.ds(0, 2)])
    low, high = pl.ds(0, LANES), pl.ds(LANES, LANES)
    hub_push(2, hubs.at[2, low], hubs.at[4, low], along_x(1))
    hub_push(2, hubs.at[6, high], hubs.at[4, high], along_x(XS - 1))
    hub_push(3, hubs.at[2], hubs.at[3], partner)
    hub_push(3, hubs.at[6], hubs.at[7], partner)
    lay_counts((1, 7))
    add_blocks((1, 7), 0)
    relay(2, 0, 0)
    relay(2, 0, 1)
    drain(recv.at[2], hubs.at[0])
    hub_push(3, hubs.at[4], hubs.at[5], partner)
    add_blocks((1, 7), 1)
    lay_counts((2, 6))
    relay(2, 1, 0)
    add_blocks((2, 6), 0)
    relay(3, 0, 0)
    lay_counts((3, 5))
    relay(2, 1, 1)
    relay(3, 0, 1)
    add_blocks((3, 5), 0)
    lay_counts((4,))
    relay(3, 1, 0)
    add_blocks((2, 6), 1)

    def finish(group):
        for half in range(2):
            drain(ag_recv.at[half, 3, group, 0], ag.at[half, 0, 0])
            add_block(half, 4, group)
            for step in (4, 3, 5, 2, 6, 1, 7):
                launch(
                    push(
                        pacc.at[half, (spot[half] + step) % RING, group], part.at[group, half, step - 1],
                        send.at[3], recv.at[4 + group], cross[half](step),
                    )
                )

    finish(0)
    relay(3, 1, 1)
    add_blocks((3, 5), 1)
    finish(1)
    drain(recv.at[3], hubs.at[pl.ds(0, 4)])
    lax.fori_loop(0, 8, hub_block, 0, unroll=True)

    product = jnp.zeros((SEEDS, 2 * LANES), jnp.float32)
    for group in range(2):
        drain(recv.at[4 + group], part.at[group])
        lines = []
        for half in range(2):
            top = half * LANES + group * WIDE
            total = tot[top : top + WIDE] + pacc[half, spot[half], group]
            for step in range(1, RING):
                total = total + part[group, half, step - 1]
            lines.append(total)
        mean = jnp.transpose(jnp.concatenate(lines, axis=0) / taken[...])
        parts = [weight[half * LANES + group * WIDE : half * LANES + (group + 1) * WIDE] for half in range(2)]
        product = product + jnp.dot(
            mean, jnp.concatenate(parts, axis=0), precision=lax.Precision.HIGHEST, preferred_element_type=jnp.float32
        )
    out[...] = jnp.maximum(product + bias[...], 0.0)
    drain(send.at[0], ag.at[:, pl.ds(0, RING - 1)])
    drain(send.at[1], meta_tx.at[:, pl.ds(0, RING - 1)])
    drain(send.at[2], hubs.at[pl.ds(0, 7)])
    drain(send.at[3], part)


def local(features, seed_self, hub_ids, requests, counts, neighbors, weight, out_bias):
    hbm = pl.BlockSpec(memory_space=pltpu.HBM)
    vmem = pl.BlockSpec(memory_space=pltpu.VMEM)
    dma = pltpu.SemaphoreType.DMA
    return pl.pallas_call(
        kernel,
        out_shape=jax.ShapeDtypeStruct((SEEDS, 2 * LANES), jnp.float32),
        in_specs=[hbm] * 8,
        out_specs=vmem,
        scratch_shapes=[
            pltpu.VMEM((ROWS, 2 * LANES), jnp.float32),
            pltpu.VMEM((SEEDS, 2 * LANES), jnp.float32),
            pltpu.VMEM((1, LANES), jnp.int32),
            pltpu.VMEM((CAP, RING * RING), jnp.int32),
            pltpu.VMEM((RING * RING, CAP), jnp.int32),
            pltpu.SMEM((RING * RING,), jnp.int32),
            pltpu.VMEM((FAN, SEEDS), jnp.int32),
            pltpu.VMEM((2 * LANES, 2 * LANES), jnp.float32),
            pltpu.VMEM((1, 2 * LANES), jnp.float32),
            dma((8,)),
            pltpu.VMEM((2, RING, 2, 2, WIDE, 2 * LANES), jnp.float32),
            pltpu.VMEM((2, RING, 24, LANES), jnp.int32),
            pltpu.VMEM((2, RING, 24, LANES), jnp.int32),
            pltpu.VMEM((2, RING, 2 * LANES), jnp.int32),
            pltpu.VMEM((2, RING, 4, LANES, 2 * LANES), jnp.bfloat16),
            pltpu.VMEM((2, RING, 2, WIDE, LANES), jnp.float32),
            pltpu.VMEM((2, 2, RING - 1, WIDE, LANES), jnp.float32),
            pltpu.VMEM((2 * XS, 2 * LANES, LANES), jnp.float32),
            pltpu.VMEM((2 * LANES, LANES), jnp.float32),
            pltpu.VMEM((1, LANES), jnp.float32),
            dma((4,)),
            dma((6,)),
            dma((2, 4, 2, 2)),
            pltpu.SemaphoreType.REGULAR((2, 2)),
        ],
        compiler_params=pltpu.CompilerParams(collective_id=0, has_side_effects=True, vmem_limit_bytes=40 * 1024 * 1024),
        name="sage",
    )(
        *(
            pltpu.with_memory_space_constraint(x, pltpu.HBM)
            for x in (
                features, seed_self, hub_ids.reshape(1, LANES), requests.T, counts, neighbors.T, weight,
                out_bias.reshape(1, 2 * LANES),
            )
        )
    )


def solution(mesh):
    rows, flat = P(("rep", "shard"), None), P(("rep", "shard"))
    return jax.shard_map(
        local, mesh=mesh, in_specs=(rows, rows, flat, rows, flat, rows, P(), P()), out_specs=rows, check_vma=False
    )
```

```python
import functools

import jax
import jax.numpy as jnp
from jax import lax
from jax.experimental import pallas as pl
from jax.experimental.pallas import tpu as pltpu
from jax.sharding import PartitionSpec as P

MESH = pl.DeviceIdType.MESH
RING = 8
XS = 4
ROWS = 512
SEEDS = 128
FAN = 15
CAP = 32
HUBS = 1024
CHUNKS = 4
LANES = 128
WIDE = 64


def split(values):
    high = values.astype(jnp.bfloat16)
    low = (values - high.astype(jnp.float32)).astype(jnp.bfloat16)
    return jnp.concatenate([high, low], axis=0)


def dot(left, right):
    return jnp.dot(left, right, preferred_element_type=jnp.float32)


def kernel(
    feat_in, own_in, hub_in, req_in, counts_in, codes_in, weight_in, bias_in, out,
    feat, own, hub_id, req_v, req, counts, codes_v, weight, bias, fetch,
    ag, meta_tx, meta_rx, ids, cblk, pacc, part, far, mix, hubs, tot, taken,
    send, recv, far_recv, ag_recv, token,
):
    rep = lax.axis_index("rep")
    shard = lax.axis_index("shard")
    me_x, core = rep // 2, rep % 2
    me = (shard % RING, shard // RING)

    def along_y(step):
        return {"rep": rep, "shard": me[1] * RING + (me[0] + step) % RING}

    def along_z(step):
        return {"rep": rep, "shard": ((me[1] + step) % RING) * RING + me[0]}

    def along_x(step):
        return {"rep": ((me_x + step) % XS) * 2 + core, "shard": shard}

    ring = (along_y, along_z)
    cross = (along_z, along_y)
    spot = (me[1], me[0])

    barrier = pltpu.get_barrier_semaphore()
    partner = {"rep": me_x * 2 + 1 - core, "shard": shard}
    peers = [along_y(1), along_y(RING - 1), along_z(1), along_z(RING - 1), along_x(1), along_x(XS - 1), partner]
    for peer in peers:
        pl.semaphore_signal(barrier, inc=1, device_id=peer, device_id_type=MESH)

    loads = []

    def load(src, dst):
        copy = pltpu.make_async_copy(src, dst, fetch.at[len(loads)])
        copy.start()
        loads.append(copy)
        return copy

    tables = load(feat_in, feat)
    small = [load(codes_in, codes_v), load(counts_in, counts), load(req_in, req_v), load(hub_in, hub_id)]
    large = [load(own_in, own), load(weight_in, weight), load(bias_in, bias)]

    def push(src, dst, send, recv, peer):
        return pltpu.make_async_remote_copy(
            src_ref=src, dst_ref=dst, send_sem=send, recv_sem=recv, device_id=peer, device_id_type=MESH
        )

    def launch(copy):
        copy.start()
        return copy

    def drain(semaphore, view):
        pltpu.make_async_copy(view, view, semaphore).wait()

    def table(half, way, wave, group, turn):
        piece = turn if way == 0 else 1 - turn
        slot_from = wave if way == 0 else (RING - wave) % RING
        slot_to = wave + 1 if way == 0 else RING - wave - 1
        return push(
            ag.at[half, slot_from, group, piece], ag.at[half, slot_to, group, piece],
            send.at[0], ag_recv.at[half, wave, group, turn],
            ring[half](1 if way == 0 else RING - 1),
        )

    def send_own(group):
        for turn in range(2):
            for half in range(2):
                for way in range(2):
                    launch(table(half, way, 0, group, turn))

    def tell(half, way):
        peer = ring[half](1 if way == 0 else RING - 1)
        pl.semaphore_signal(token.at[half, way], inc=1, device_id=peer, device_id_type=MESH)

    cblk[...] = jnp.zeros_like(cblk)
    tables.wait()
    for chunk in range(CHUNKS):
        for half in range(2):
            block = jnp.transpose(feat[chunk * LANES : (chunk + 1) * LANES, half * LANES : (half + 1) * LANES])
            left = (chunk % 2) * LANES
            for group in range(2):
                ag[half, 0, group, chunk // 2, :, left : left + LANES] = block[group * WIDE : (group + 1) * WIDE]
    pl.semaphore_wait(barrier, len(peers))
    for half in range(2):
        for way in range(2):
            tell(half, way)
    send_own(0)

    for copy in small:
        copy.wait()
    codes = jnp.concatenate([codes_v[...], jnp.full((1, LANES), -1, jnp.int32)], axis=0)
    owner = (codes - HUBS) >> 5
    slot = (codes - HUBS) & 31

    def look(d, found):
        return jnp.where(owner == d, counts[d], found)

    filled = lax.fori_loop(0, RING * RING, look, jnp.zeros_like(codes), unroll=8)
    live = (codes >= 0) & ((codes < HUBS) | (slot < filled))
    codes = jnp.where(live, codes, -1)
    taken[...] = 1.0 + jnp.sum(live.astype(jnp.float32), axis=0, keepdims=True)
    req[...] = jnp.transpose(req_v[...])
    lane = lax.broadcasted_iota(jnp.int32, (RING, LANES), 1) // CAP
    for half in range(2):
        for place in range(RING):
            if half == 0:
                lists = req[place * RING : (place + 1) * RING]
            else:
                lists = req[pl.ds(place, RING, stride=RING)]
            lists = jnp.concatenate([lists] * 4, axis=1)
            meta_tx[half, place, 0:16] = codes
            meta_tx[half, place, 16:24] = jnp.where(lane == spot[half] % 4, lists, 0)
        meta_rx[half, spot[half], 0:16] = codes
    for half in range(2):
        meta_rx[half, spot[half], 16:24] = meta_tx[half, spot[half], 16:24]

    for hop in range(3):
        for way in range(2):
            for half in range(2):
                if hop < 2 or way == 0:
                    pl.semaphore_wait(token.at[half, way], 1)
                    if hop + way < 2:
                        tell(half, way)

    for step in (4, 3, 5, 2, 6, 1, 7):
        for half in range(2):
            place = (spot[half] + step) % RING
            copy = push(
                meta_tx.at[half, place], meta_rx.at[half, spot[half]],
                send.at[1], recv.at[0], cross[half](step),
            )
            launch(copy)
    send_own(1)

    hub_sum = jnp.zeros((4 * LANES, LANES), jnp.float32)
    for piece in range(2):
        block = jnp.concatenate([ag[half, 0, group, piece] for half in range(2) for group in range(2)], axis=0)
        rows = lax.broadcasted_iota(jnp.int32, (2 * LANES, LANES), 0) + piece * 2 * LANES
        pick = jnp.where(rows == hub_id[...], 1.0, 0.0).astype(jnp.bfloat16)
        hub_sum = hub_sum + dot(split(block), pick)
    hubs[0] = hub_sum[: 2 * LANES] + hub_sum[2 * LANES :]

    def hub_push(index, src, dst, peer):
        launch(push(src, dst, send.at[2], recv.at[index], peer))

    hub_push(1, hubs.at[0], hubs.at[2], along_x(1))
    hub_push(1, hubs.at[0], hubs.at[6], along_x(XS - 1))
    hub_push(3, hubs.at[0], hubs.at[1], partner)

    for copy in large:
        copy.wait()
    tot[...] = jnp.transpose(own[...])

    def relay(wave, group, turn):
        for half in range(2):
            drain(ag_recv.at[half, wave - 1, group, turn], ag.at[half, 0, 0])
            if wave < 3 or turn == 0:
                for way in range(2):
                    launch(table(half, way, wave, group, turn))

    def place_of(half, slot_index):
        return (me[half] + RING - slot_index) % RING

    def lay_counts(slots):
        for half in range(2):
            for slot_index in slots:
                origin = place_of(half, slot_index)
                number = me[1] * RING + origin if half == 0 else origin * RING + me[0]
                lines = lax.broadcasted_iota(jnp.int32, (CAP, LANES), 0) + (HUBS + number * CAP)
                for place in range(RING):
                    count = jnp.zeros((CAP, LANES), jnp.float32)
                    for k in range(FAN):
                        count = count + jnp.where(meta_rx[half, place, k : k + 1] == lines, 1.0, 0.0)
                    top, left = CAP * (place % 4), LANES * (place % 2)
                    cblk[half, slot_index, place // 2, top : top + CAP, left : left + LANES] = count.astype(jnp.bfloat16)

    def add_block(half, slot_index, group):
        block = jnp.concatenate([ag[half, slot_index, group, piece] for piece in range(2)], axis=1)
        wanted = ids[half, pl.ds(place_of(half, slot_index), 1), :]
        rows = lax.broadcasted_iota(jnp.int32, (ROWS, 2 * LANES), 0)
        found = dot(split(block), jnp.where(rows == wanted, 1.0, 0.0).astype(jnp.bfloat16)).astype(jnp.bfloat16)
        for pair in range(RING // 2):
            side = (pair // 2) * LANES
            sums = dot(found[:, side : side + LANES], cblk[half, slot_index, pair])
            sums = sums[:WIDE] + sums[WIDE:]
            for k in range(2):
                piece = sums[:, k * LANES : (k + 1) * LANES]
                if slot_index == 0:
                    pacc[half, 2 * pair + k, group] = piece
                else:
                    pacc[half, 2 * pair + k, group] += piece

    def add_blocks(slots, group):
        for slot_index in slots:
            for half in range(2):
                add_block(half, slot_index, group)

    def hub_block(index, carry):
        chip, over = index // 2, index % 2
        origin = ((me_x + XS - chip) % XS) * 2 + (core + over) % 2
        lines = lax.broadcasted_iota(jnp.int32, (LANES, LANES), 0) + origin * LANES
        mine = spot[0]
        count = jnp.zeros((LANES, LANES), jnp.float32)
        for k in range(FAN):
            count = count + jnp.where(meta_rx[0, mine, k : k + 1] == lines, 1.0, 0.0)
        sums = dot(split(hubs[index]), count.astype(jnp.bfloat16))
        tot[...] += sums[: 2 * LANES] + sums[2 * LANES :]
        return carry

    relay(1, 0, 0)
    relay(1, 0, 1)
    drain(recv.at[0], meta_rx.at[:, pl.ds(0, RING - 1)])
    for half in range(2):
        for group in range(2):
            tiles = [meta_rx[half, 4 * group + k, 16:24] for k in range(4)]
            ids[half, :, group * LANES : (group + 1) * LANES] = tiles[0] + tiles[1] + tiles[2] + tiles[3]
    lay_counts((0,))
    add_blocks((0,), 0)
    add_blocks((0,), 1)
    relay(1, 1, 0)
    relay(1, 1, 1)
    drain(recv.at[1], hubs.at[pl.ds(0, 2)])
    low, high = pl.ds(0, LANES), pl.ds(LANES, LANES)
    hub_push(2, hubs.at[2, low], hubs.at[4, low], along_x(1))
    hub_push(2, hubs.at[6, high], hubs.at[4, high], along_x(XS - 1))
    hub_push(3, hubs.at[2], hubs.at[3], partner)
    hub_push(3, hubs.at[6], hubs.at[7], partner)
    lay_counts((1, 7))
    add_blocks((1, 7), 0)
    relay(2, 0, 0)
    relay(2, 0, 1)
    drain(recv.at[2], hubs.at[0])
    hub_push(3, hubs.at[4], hubs.at[5], partner)
    add_blocks((1, 7), 1)
    lay_counts((2, 6))
    relay(2, 1, 0)
    add_blocks((2, 6), 0)
    relay(3, 0, 0)
    lay_counts((3, 5))
    relay(2, 1, 1)
    relay(3, 0, 1)
    add_blocks((3, 5), 0)
    lay_counts((4,))
    relay(3, 1, 0)
    add_blocks((2, 6), 1)

    def finish(group):
        for half in range(2):
            drain(ag_recv.at[half, 3, group, 0], ag.at[half, 0, 0])
            add_block(half, 4, group)
            here = spot[half]
            for way in range(2):
                sign = 1 - 2 * way
                third = pacc.at[half, (here + 3 * sign + RING) % RING, group]
                fourth = pacc.at[half, (here + 4) % RING, group, pl.ds(way * WIDE // 2, WIDE // 2)]
                launch(
                    push(
                        fourth, far.at[group, half, way, pl.ds(WIDE, WIDE // 2)],
                        send.at[3], far_recv.at[group, half], cross[half]((2 * sign) % RING),
                    )
                )
                launch(
                    push(
                        third, far.at[group, half, way, pl.ds(0, WIDE)],
                        send.at[3], far_recv.at[group, half], cross[half](sign % RING),
                    )
                )
            for way in range(2):
                sign = 1 - 2 * way
                first = pacc.at[half, (here + sign + RING) % RING, group]
                launch(push(first, part.at[group, half, way], send.at[4], recv.at[4 + group], cross[half](sign % RING)))

    def combine(group):
        for half in range(2):
            drain(far_recv.at[group, half], far.at[group, half])
            for way in range(2):
                sign = 1 - 2 * way
                rest = jnp.zeros((WIDE // 2, LANES), jnp.float32)
                piece = far[group, half, way, WIDE:]
                piece = jnp.concatenate([piece, rest] if way == 0 else [rest, piece], axis=0)
                mine = pacc[half, (spot[half] + 2 * sign + RING) % RING, group]
                mix[group, half, way] = mine + far[group, half, way, :WIDE] + piece
                launch(
                    push(
                        mix.at[group, half, way], part.at[group, half, 2 + way],
                        send.at[4], recv.at[4 + group], cross[half]((2 * sign) % RING),
                    )
                )

    finish(0)
    relay(3, 1, 1)
    add_blocks((3, 5), 1)
    finish(1)
    combine(0)
    drain(recv.at[3], hubs.at[pl.ds(0, 4)])
    lax.fori_loop(0, 8, hub_block, 0, unroll=True)
    combine(1)

    product = jnp.zeros((SEEDS, 2 * LANES), jnp.float32)
    for group in range(2):
        drain(recv.at[4 + group], part.at[group])
        lines = []
        for half in range(2):
            top = half * LANES + group * WIDE
            total = tot[top : top + WIDE] + pacc[half, spot[half], group]
            for source in range(4):
                total = total + part[group, half, source]
            lines.append(total)
        mean = jnp.transpose(jnp.concatenate(lines, axis=0) / taken[...])
        parts = [weight[half * LANES + group * WIDE : half * LANES + (group + 1) * WIDE] for half in range(2)]
        product = product + jnp.dot(
            mean, jnp.concatenate(parts, axis=0), precision=lax.Precision.HIGHEST, preferred_element_type=jnp.float32
        )
    out[...] = jnp.maximum(product + bias[...], 0.0)
    drain(send.at[0], ag.at[:, pl.ds(0, RING - 1)])
    drain(send.at[1], meta_tx.at[:, pl.ds(0, RING - 1)])
    drain(send.at[2], hubs.at[pl.ds(0, 7)])
    drain(send.at[3], far)
    drain(send.at[4], part)


def local(features, seed_self, hub_ids, requests, counts, neighbors, weight, out_bias):
    hbm = pl.BlockSpec(memory_space=pltpu.HBM)
    vmem = pl.BlockSpec(memory_space=pltpu.VMEM)
    dma = pltpu.SemaphoreType.DMA
    return pl.pallas_call(
        kernel,
        out_shape=jax.ShapeDtypeStruct((SEEDS, 2 * LANES), jnp.float32),
        in_specs=[hbm] * 8,
        out_specs=vmem,
        scratch_shapes=[
            pltpu.VMEM((ROWS, 2 * LANES), jnp.float32),
            pltpu.VMEM((SEEDS, 2 * LANES), jnp.float32),
            pltpu.VMEM((1, LANES), jnp.int32),
            pltpu.VMEM((CAP, RING * RING), jnp.int32),
            pltpu.VMEM((RING * RING, CAP), jnp.int32),
            pltpu.SMEM((RING * RING,), jnp.int32),
            pltpu.VMEM((FAN, SEEDS), jnp.int32),
            pltpu.VMEM((2 * LANES, 2 * LANES), jnp.float32),
            pltpu.VMEM((1, 2 * LANES), jnp.float32),
            dma((8,)),
            pltpu.VMEM((2, RING, 2, 2, WIDE, 2 * LANES), jnp.float32),
            pltpu.VMEM((2, RING, 24, LANES), jnp.int32),
            pltpu.VMEM((2, RING, 24, LANES), jnp.int32),
            pltpu.VMEM((2, RING, 2 * LANES), jnp.int32),
            pltpu.VMEM((2, RING, 4, LANES, 2 * LANES), jnp.bfloat16),
            pltpu.VMEM((2, RING, 2, WIDE, LANES), jnp.float32),
            pltpu.VMEM((2, 2, 4, WIDE, LANES), jnp.float32),
            pltpu.VMEM((2, 2, 2, WIDE + WIDE // 2, LANES), jnp.float32),
            pltpu.VMEM((2, 2, 2, WIDE, LANES), jnp.float32),
            pltpu.VMEM((2 * XS, 2 * LANES, LANES), jnp.float32),
            pltpu.VMEM((2 * LANES, LANES), jnp.float32),
            pltpu.VMEM((1, LANES), jnp.float32),
            dma((5,)),
            dma((6,)),
            dma((2, 2)),
            dma((2, 4, 2, 2)),
            pltpu.SemaphoreType.REGULAR((2, 2)),
        ],
        compiler_params=pltpu.CompilerParams(collective_id=0, has_side_effects=True, vmem_limit_bytes=40 * 1024 * 1024),
        name="sage",
    )(
        *(
            pltpu.with_memory_space_constraint(x, pltpu.HBM)
            for x in (
                features, seed_self, hub_ids.reshape(1, LANES), requests.T, counts, neighbors.T, weight,
                out_bias.reshape(1, 2 * LANES),
            )
        )
    )


def solution(mesh):
    rows, flat = P(("rep", "shard"), None), P(("rep", "shard"))
    return jax.shard_map(
        local, mesh=mesh, in_specs=(rows, rows, flat, rows, flat, rows, P(), P()), out_specs=rows, check_vma=False
    )
```

```python
import functools

import jax
import jax.numpy as jnp
from jax import lax
from jax.experimental import pallas as pl
from jax.experimental.pallas import tpu as pltpu
from jax.sharding import PartitionSpec as P

MESH = pl.DeviceIdType.MESH
RING = 8
XS = 4
ROWS = 512
SEEDS = 128
FAN = 15
CAP = 32
HUBS = 1024
CHUNKS = 4
LANES = 128
WIDE = 64
META = 18


def split(values):
    high = values.astype(jnp.bfloat16)
    low = (values - high.astype(jnp.float32)).astype(jnp.bfloat16)
    return jnp.concatenate([high, low], axis=0)


def dot(left, right):
    return jnp.dot(left, right, preferred_element_type=jnp.float32)


def kernel(
    feat_in, own_in, hub_in, req_in, counts_in, codes_in, weight_in, bias_in, out,
    feat, own, hub_id, req_v, req, counts, codes_v, weight, bias, fetch,
    ag, meta_tx, meta_rx, ids, cblk, pacc, part, far, mix, hubs, tot, taken,
    send, recv, far_recv, ag_recv, token,
):
    rep = lax.axis_index("rep")
    shard = lax.axis_index("shard")
    me_x, core = rep // 2, rep % 2
    me = (shard % RING, shard // RING)

    def along_y(step):
        return {"rep": rep, "shard": me[1] * RING + (me[0] + step) % RING}

    def along_z(step):
        return {"rep": rep, "shard": ((me[1] + step) % RING) * RING + me[0]}

    def along_x(step):
        return {"rep": ((me_x + step) % XS) * 2 + core, "shard": shard}

    ring = (along_y, along_z)
    cross = (along_z, along_y)
    spot = (me[1], me[0])

    barrier = pltpu.get_barrier_semaphore()
    partner = {"rep": me_x * 2 + 1 - core, "shard": shard}
    peers = [along_y(1), along_y(RING - 1), along_z(1), along_z(RING - 1), along_x(1), along_x(XS - 1), partner]
    for peer in peers:
        pl.semaphore_signal(barrier, inc=1, device_id=peer, device_id_type=MESH)

    loads = []

    def load(src, dst):
        copy = pltpu.make_async_copy(src, dst, fetch.at[len(loads)])
        copy.start()
        loads.append(copy)
        return copy

    tables = load(feat_in, feat)
    small = [load(codes_in, codes_v), load(counts_in, counts), load(req_in, req_v), load(hub_in, hub_id)]
    large = [load(own_in, own), load(weight_in, weight), load(bias_in, bias)]

    def push(src, dst, send, recv, peer):
        return pltpu.make_async_remote_copy(
            src_ref=src, dst_ref=dst, send_sem=send, recv_sem=recv, device_id=peer, device_id_type=MESH
        )

    def launch(copy):
        copy.start()
        return copy

    def drain(semaphore, view):
        pltpu.make_async_copy(view, view, semaphore).wait()

    def table(half, way, wave, group, turn):
        piece = turn if way == 0 else 1 - turn
        slot_from = wave if way == 0 else (RING - wave) % RING
        slot_to = wave + 1 if way == 0 else RING - wave - 1
        return push(
            ag.at[half, slot_from, group, piece], ag.at[half, slot_to, group, piece],
            send.at[0], ag_recv.at[half, wave, group, turn],
            ring[half](1 if way == 0 else RING - 1),
        )

    def send_own(group):
        for turn in range(2):
            for half in range(2):
                for way in range(2):
                    launch(table(half, way, 0, group, turn))

    def tell(half, way):
        peer = ring[half](1 if way == 0 else RING - 1)
        pl.semaphore_signal(token.at[half, way], inc=1, device_id=peer, device_id_type=MESH)

    cblk[...] = jnp.zeros_like(cblk)
    tables.wait()
    for chunk in range(CHUNKS):
        for half in range(2):
            block = jnp.transpose(feat[chunk * LANES : (chunk + 1) * LANES, half * LANES : (half + 1) * LANES])
            left = (chunk % 2) * LANES
            for group in range(2):
                ag[half, 0, group, chunk // 2, :, left : left + LANES] = block[group * WIDE : (group + 1) * WIDE]
    pl.semaphore_wait(barrier, len(peers))
    for half in range(2):
        for way in range(2):
            tell(half, way)
    send_own(0)

    for copy in small:
        copy.wait()
    codes = jnp.concatenate([codes_v[...], jnp.full((1, LANES), -1, jnp.int32)], axis=0)
    owner = (codes - HUBS) >> 5
    slot = (codes - HUBS) & 31

    def look(d, found):
        return jnp.where(owner == d, counts[d], found)

    filled = lax.fori_loop(0, RING * RING, look, jnp.zeros_like(codes), unroll=8)
    live = (codes >= 0) & ((codes < HUBS) | (slot < filled))
    codes = jnp.where(live, codes, -1)
    taken[...] = 1.0 + jnp.sum(live.astype(jnp.float32), axis=0, keepdims=True)
    req[...] = jnp.transpose(req_v[...])
    packed = jnp.concatenate([req[pl.ds(p, 2 * RING, stride=4)] for p in range(4)], axis=1)
    upper, lower = (
        jnp.concatenate([req[(4 * h + p) * RING : (4 * h + p + 1) * RING] for p in range(4)], axis=1) for h in range(2)
    )
    for place in range(RING):
        for half in range(2):
            meta_tx[half, place, 0:16] = codes
        meta_tx[0, place, 16:18] = packed[2 * place : 2 * place + 2]
        meta_tx[1, place, 16:17] = upper[place : place + 1]
        meta_tx[1, place, 17:18] = lower[place : place + 1]
    for half in range(2):
        meta_rx[half, spot[half], 0:16] = codes
        meta_rx[half, spot[half], 16:18] = meta_tx[half, spot[half], 16:18]

    for hop in range(3):
        for way in range(2):
            for half in range(2):
                if hop < 2 or way == 0:
                    pl.semaphore_wait(token.at[half, way], 1)
                    if hop + way < 2:
                        tell(half, way)

    for step in (4, 3, 5, 2, 6, 1, 7):
        for half in range(2):
            place = (spot[half] + step) % RING
            copy = push(
                meta_tx.at[half, place, pl.ds(0, META)], meta_rx.at[half, spot[half], pl.ds(0, META)],
                send.at[1], recv.at[0], cross[half](step),
            )
            launch(copy)
    send_own(1)

    hub_sum = jnp.zeros((4 * LANES, LANES), jnp.float32)
    for piece in range(2):
        block = jnp.concatenate([ag[half, 0, group, piece] for half in range(2) for group in range(2)], axis=0)
        rows = lax.broadcasted_iota(jnp.int32, (2 * LANES, LANES), 0) + piece * 2 * LANES
        pick = jnp.where(rows == hub_id[...], 1.0, 0.0).astype(jnp.bfloat16)
        hub_sum = hub_sum + dot(split(block), pick)
    hubs[0] = hub_sum[: 2 * LANES] + hub_sum[2 * LANES :]

    def hub_push(index, src, dst, peer):
        launch(push(src, dst, send.at[2], recv.at[index], peer))

    hub_push(1, hubs.at[0], hubs.at[2], along_x(1))
    hub_push(1, hubs.at[0], hubs.at[6], along_x(XS - 1))
    hub_push(3, hubs.at[0], hubs.at[1], partner)

    for copy in large:
        copy.wait()
    tot[...] = jnp.transpose(own[...])

    def relay(wave, group, turn):
        for half in range(2):
            drain(ag_recv.at[half, wave - 1, group, turn], ag.at[half, 0, 0])
            if wave < 3 or turn == 0:
                for way in range(2):
                    launch(table(half, way, wave, group, turn))

    def place_of(half, slot_index):
        return (me[half] + RING - slot_index) % RING

    def lay_counts(slots):
        for half in range(2):
            for slot_index in slots:
                origin = place_of(half, slot_index)
                number = me[1] * RING + origin if half == 0 else origin * RING + me[0]
                lines = lax.broadcasted_iota(jnp.int32, (CAP, LANES), 0) + (HUBS + number * CAP)
                for place in range(RING):
                    count = jnp.zeros((CAP, LANES), jnp.float32)
                    for k in range(FAN):
                        count = count + jnp.where(meta_rx[half, place, k : k + 1] == lines, 1.0, 0.0)
                    top, left = CAP * (place % 4), LANES * (place % 2)
                    cblk[half, slot_index, place // 2, top : top + CAP, left : left + LANES] = count.astype(jnp.bfloat16)

    def add_block(half, slot_index, group):
        block = jnp.concatenate([ag[half, slot_index, group, piece] for piece in range(2)], axis=1)
        wanted = ids[half, pl.ds(place_of(half, slot_index), 1), :]
        rows = lax.broadcasted_iota(jnp.int32, (ROWS, 2 * LANES), 0)
        found = dot(split(block), jnp.where(rows == wanted, 1.0, 0.0).astype(jnp.bfloat16)).astype(jnp.bfloat16)
        for pair in range(RING // 2):
            side = (pair // 2) * LANES
            sums = dot(found[:, side : side + LANES], cblk[half, slot_index, pair])
            sums = sums[:WIDE] + sums[WIDE:]
            for k in range(2):
                piece = sums[:, k * LANES : (k + 1) * LANES]
                if slot_index == 0:
                    pacc[half, 2 * pair + k, group] = piece
                else:
                    pacc[half, 2 * pair + k, group] += piece

    def add_blocks(slots, group):
        for slot_index in slots:
            for half in range(2):
                add_block(half, slot_index, group)

    def hub_block(index, carry):
        chip, over = index // 2, index % 2
        origin = ((me_x + XS - chip) % XS) * 2 + (core + over) % 2
        lines = lax.broadcasted_iota(jnp.int32, (LANES, LANES), 0) + origin * LANES
        mine = spot[0]
        count = jnp.zeros((LANES, LANES), jnp.float32)
        for k in range(FAN):
            count = count + jnp.where(meta_rx[0, mine, k : k + 1] == lines, 1.0, 0.0)
        sums = dot(split(hubs[index]), count.astype(jnp.bfloat16))
        tot[...] += sums[: 2 * LANES] + sums[2 * LANES :]
        return carry

    relay(1, 0, 0)
    relay(1, 0, 1)
    drain(recv.at[0], meta_rx.at[:, pl.ds(0, RING - 1), pl.ds(0, META)])
    set_of = lax.broadcasted_iota(jnp.int32, (2, LANES), 1) // CAP
    for half in range(2):
        for group in range(2):
            lists = [meta_rx[half, 4 * group + k, 16:18] for k in range(4)]
            for p in range(4):
                row = jnp.zeros((2, LANES), jnp.int32)
                for k in range(4):
                    taken_set = jnp.where(set_of == p, lists[k], 0)
                    row = row + (pltpu.roll(taken_set, ((k - p) % 4) * CAP, 1) if k != p else taken_set)
                ids[half, p : p + 1, group * LANES : (group + 1) * LANES] = row[0:1]
                ids[half, 4 + p : 5 + p, group * LANES : (group + 1) * LANES] = row[1:2]
    lay_counts((0,))
    add_blocks((0,), 0)
    add_blocks((0,), 1)
    relay(1, 1, 0)
    relay(1, 1, 1)
    drain(recv.at[1], hubs.at[pl.ds(0, 2)])
    low, high = pl.ds(0, LANES), pl.ds(LANES, LANES)
    hub_push(2, hubs.at[2, low], hubs.at[4, low], along_x(1))
    hub_push(2, hubs.at[6, high], hubs.at[4, high], along_x(XS - 1))
    hub_push(3, hubs.at[2], hubs.at[3], partner)
    hub_push(3, hubs.at[6], hubs.at[7], partner)
    lay_counts((1, 7))
    add_blocks((1, 7), 0)
    relay(2, 0, 0)
    relay(2, 0, 1)
    drain(recv.at[2], hubs.at[0])
    hub_push(3, hubs.at[4], hubs.at[5], partner)
    add_blocks((1, 7), 1)
    lay_counts((2, 6))
    relay(2, 1, 0)
    add_blocks((2, 6), 0)
    relay(3, 0, 0)
    lay_counts((3, 5))
    relay(2, 1, 1)
    relay(3, 0, 1)
    add_blocks((3, 5), 0)
    lay_counts((4,))
    relay(3, 1, 0)
    add_blocks((2, 6), 1)

    def finish(group):
        for half in range(2):
            drain(ag_recv.at[half, 3, group, 0], ag.at[half, 0, 0])
            add_block(half, 4, group)
            here = spot[half]
            for way in range(2):
                sign = 1 - 2 * way
                third = pacc.at[half, (here + 3 * sign + RING) % RING, group]
                fourth = pacc.at[half, (here + 4) % RING, group, pl.ds(way * WIDE // 2, WIDE // 2)]
                launch(
                    push(
                        fourth, far.at[group, half, way, pl.ds(WIDE, WIDE // 2)],
                        send.at[3], far_recv.at[group, half], cross[half]((2 * sign) % RING),
                    )
                )
                launch(
                    push(
                        third, far.at[group, half, way, pl.ds(0, WIDE)],
                        send.at[3], far_recv.at[group, half], cross[half](sign % RING),
                    )
                )
            for way in range(2):
                sign = 1 - 2 * way
                first = pacc.at[half, (here + sign + RING) % RING, group]
                launch(push(first, part.at[group, half, way], send.at[4], recv.at[4 + group], cross[half](sign % RING)))

    def combine(group):
        for half in range(2):
            drain(far_recv.at[group, half], far.at[group, half])
            for way in range(2):
                sign = 1 - 2 * way
                rest = jnp.zeros((WIDE // 2, LANES), jnp.float32)
                piece = far[group, half, way, WIDE:]
                piece = jnp.concatenate([piece, rest] if way == 0 else [rest, piece], axis=0)
                mine = pacc[half, (spot[half] + 2 * sign + RING) % RING, group]
                mix[group, half, way] = mine + far[group, half, way, :WIDE] + piece
                launch(
                    push(
                        mix.at[group, half, way], part.at[group, half, 2 + way],
                        send.at[4], recv.at[4 + group], cross[half]((2 * sign) % RING),
                    )
                )

    finish(0)
    relay(3, 1, 1)
    add_blocks((3, 5), 1)
    finish(1)
    combine(0)
    drain(recv.at[3], hubs.at[pl.ds(0, 4)])
    lax.fori_loop(0, 8, hub_block, 0, unroll=True)
    combine(1)

    product = jnp.zeros((SEEDS, 2 * LANES), jnp.float32)
    for group in range(2):
        drain(recv.at[4 + group], part.at[group])
        lines = []
        for half in range(2):
            top = half * LANES + group * WIDE
            total = tot[top : top + WIDE] + pacc[half, spot[half], group]
            for source in range(4):
                total = total + part[group, half, source]
            lines.append(total)
        mean = jnp.transpose(jnp.concatenate(lines, axis=0) / taken[...])
        parts = [weight[half * LANES + group * WIDE : half * LANES + (group + 1) * WIDE] for half in range(2)]
        product = product + jnp.dot(
            mean, jnp.concatenate(parts, axis=0), precision=lax.Precision.HIGHEST, preferred_element_type=jnp.float32
        )
    out[...] = jnp.maximum(product + bias[...], 0.0)
    drain(send.at[0], ag.at[:, pl.ds(0, RING - 1)])
    drain(send.at[1], meta_tx.at[:, pl.ds(0, RING - 1), pl.ds(0, META)])
    drain(send.at[2], hubs.at[pl.ds(0, 7)])
    drain(send.at[3], far)
    drain(send.at[4], part)


def local(features, seed_self, hub_ids, requests, counts, neighbors, weight, out_bias):
    hbm = pl.BlockSpec(memory_space=pltpu.HBM)
    vmem = pl.BlockSpec(memory_space=pltpu.VMEM)
    dma = pltpu.SemaphoreType.DMA
    return pl.pallas_call(
        kernel,
        out_shape=jax.ShapeDtypeStruct((SEEDS, 2 * LANES), jnp.float32),
        in_specs=[hbm] * 8,
        out_specs=vmem,
        scratch_shapes=[
            pltpu.VMEM((ROWS, 2 * LANES), jnp.float32),
            pltpu.VMEM((SEEDS, 2 * LANES), jnp.float32),
            pltpu.VMEM((1, LANES), jnp.int32),
            pltpu.VMEM((CAP, RING * RING), jnp.int32),
            pltpu.VMEM((RING * RING, CAP), jnp.int32),
            pltpu.SMEM((RING * RING,), jnp.int32),
            pltpu.VMEM((FAN, SEEDS), jnp.int32),
            pltpu.VMEM((2 * LANES, 2 * LANES), jnp.float32),
            pltpu.VMEM((1, 2 * LANES), jnp.float32),
            dma((8,)),
            pltpu.VMEM((2, RING, 2, 2, WIDE, 2 * LANES), jnp.float32),
            pltpu.VMEM((2, RING, 24, LANES), jnp.int32),
            pltpu.VMEM((2, RING, 24, LANES), jnp.int32),
            pltpu.VMEM((2, RING, 2 * LANES), jnp.int32),
            pltpu.VMEM((2, RING, 4, LANES, 2 * LANES), jnp.bfloat16),
            pltpu.VMEM((2, RING, 2, WIDE, LANES), jnp.float32),
            pltpu.VMEM((2, 2, 4, WIDE, LANES), jnp.float32),
            pltpu.VMEM((2, 2, 2, WIDE + WIDE // 2, LANES), jnp.float32),
            pltpu.VMEM((2, 2, 2, WIDE, LANES), jnp.float32),
            pltpu.VMEM((2 * XS, 2 * LANES, LANES), jnp.float32),
            pltpu.VMEM((2 * LANES, LANES), jnp.float32),
            pltpu.VMEM((1, LANES), jnp.float32),
            dma((5,)),
            dma((6,)),
            dma((2, 2)),
            dma((2, 4, 2, 2)),
            pltpu.SemaphoreType.REGULAR((2, 2)),
        ],
        compiler_params=pltpu.CompilerParams(collective_id=0, has_side_effects=True, vmem_limit_bytes=40 * 1024 * 1024),
        name="sage",
    )(
        *(
            pltpu.with_memory_space_constraint(x, pltpu.HBM)
            for x in (
                features, seed_self, hub_ids.reshape(1, LANES), requests.T, counts, neighbors.T, weight,
                out_bias.reshape(1, 2 * LANES),
            )
        )
    )


def solution(mesh):
    rows, flat = P(("rep", "shard"), None), P(("rep", "shard"))
    return jax.shard_map(
        local, mesh=mesh, in_specs=(rows, rows, flat, rows, flat, rows, P(), P()), out_specs=rows, check_vma=False
    )
```

```python
import functools

import jax
import jax.numpy as jnp
from jax import lax
from jax.experimental import pallas as pl
from jax.experimental.pallas import tpu as pltpu
from jax.sharding import PartitionSpec as P

MESH = pl.DeviceIdType.MESH
RING = 8
XS = 4
ROWS = 512
SEEDS = 128
FAN = 15
CAP = 32
HUBS = 1024
CHUNKS = 4
LANES = 128
WIDE = 64
META = 18


def split(values):
    high = values.astype(jnp.bfloat16)
    low = (values - high.astype(jnp.float32)).astype(jnp.bfloat16)
    return jnp.concatenate([high, low], axis=0)


def dot(left, right):
    return jnp.dot(left, right, preferred_element_type=jnp.float32)


def kernel(
    feat_in, own_in, hub_in, req_in, counts_in, codes_in, weight_in, bias_in, out,
    feat, own, hub_id, req_v, req, counts, codes_v, weight, bias, fetch,
    ag, meta_tx, meta_rx, ids, cblk, pacc, part, far, mix, hubs, tot, taken,
    send, recv, far_recv, ag_recv, token,
):
    rep = lax.axis_index("rep")
    shard = lax.axis_index("shard")
    me_x, core = rep // 2, rep % 2
    me = (shard % RING, shard // RING)

    def along_y(step):
        return {"rep": rep, "shard": me[1] * RING + (me[0] + step) % RING}

    def along_z(step):
        return {"rep": rep, "shard": ((me[1] + step) % RING) * RING + me[0]}

    def along_x(step):
        return {"rep": ((me_x + step) % XS) * 2 + core, "shard": shard}

    ring = (along_y, along_z)
    cross = (along_z, along_y)
    spot = (me[1], me[0])

    barrier = pltpu.get_barrier_semaphore()
    partner = {"rep": me_x * 2 + 1 - core, "shard": shard}
    peers = [along_y(1), along_y(RING - 1), along_z(1), along_z(RING - 1), along_x(1), along_x(XS - 1), partner]
    for peer in peers:
        pl.semaphore_signal(barrier, inc=1, device_id=peer, device_id_type=MESH)

    loads = []

    def load(src, dst):
        copy = pltpu.make_async_copy(src, dst, fetch.at[len(loads)])
        copy.start()
        loads.append(copy)
        return copy

    tables = load(feat_in, feat)
    small = [load(codes_in, codes_v), load(counts_in, counts), load(req_in, req_v), load(hub_in, hub_id)]
    large = [load(own_in, own), load(weight_in, weight), load(bias_in, bias)]

    def push(src, dst, send, recv, peer):
        return pltpu.make_async_remote_copy(
            src_ref=src, dst_ref=dst, send_sem=send, recv_sem=recv, device_id=peer, device_id_type=MESH
        )

    def launch(copy):
        copy.start()
        return copy

    def drain(semaphore, view):
        pltpu.make_async_copy(view, view, semaphore).wait()

    def table(half, way, wave, group, turn):
        piece = turn if way == 0 else 1 - turn
        slot_from = wave if way == 0 else (RING - wave) % RING
        slot_to = wave + 1 if way == 0 else RING - wave - 1
        return push(
            ag.at[half, slot_from, group, piece], ag.at[half, slot_to, group, piece],
            send.at[0], ag_recv.at[half, wave, group, turn],
            ring[half](1 if way == 0 else RING - 1),
        )

    def send_own(group):
        for turn in range(2):
            for half in range(2):
                for way in range(2):
                    launch(table(half, way, 0, group, turn))

    def tell(half, way):
        peer = ring[half](1 if way == 0 else RING - 1)
        pl.semaphore_signal(token.at[half, way], inc=1, device_id=peer, device_id_type=MESH)

    cblk[...] = jnp.zeros_like(cblk)
    tables.wait()
    for chunk in range(CHUNKS):
        for half in range(2):
            block = jnp.transpose(feat[chunk * LANES : (chunk + 1) * LANES, half * LANES : (half + 1) * LANES])
            left = (chunk % 2) * LANES
            for group in range(2):
                ag[half, 0, group, chunk // 2, :, left : left + LANES] = block[group * WIDE : (group + 1) * WIDE]
    pl.semaphore_wait(barrier, len(peers))
    for half in range(2):
        for way in range(2):
            tell(half, way)
    send_own(0)

    for copy in small:
        copy.wait()
    codes = jnp.concatenate([codes_v[...], jnp.full((1, LANES), -1, jnp.int32)], axis=0)
    owner = (codes - HUBS) >> 5
    slot = (codes - HUBS) & 31

    def look(d, found):
        return jnp.where(owner == d, counts[d], found)

    filled = lax.fori_loop(0, RING * RING, look, jnp.zeros_like(codes), unroll=8)
    live = (codes >= 0) & ((codes < HUBS) | (slot < filled))
    codes = jnp.where(live, codes, -1)
    taken[...] = 1.0 + jnp.sum(live.astype(jnp.float32), axis=0, keepdims=True)
    req[...] = jnp.transpose(req_v[...])
    packed = jnp.concatenate([req[pl.ds(p, 2 * RING, stride=4)] for p in range(4)], axis=1)
    upper, lower = (
        jnp.concatenate([req[(4 * h + p) * RING : (4 * h + p + 1) * RING] for p in range(4)], axis=1) for h in range(2)
    )
    for place in range(RING):
        for half in range(2):
            meta_tx[half, place, 0:16] = codes
        meta_tx[0, place, 16:18] = packed[2 * place : 2 * place + 2]
        meta_tx[1, place, 16:17] = upper[place : place + 1]
        meta_tx[1, place, 17:18] = lower[place : place + 1]
    for half in range(2):
        meta_rx[half, spot[half], 0:16] = codes
        meta_rx[half, spot[half], 16:18] = meta_tx[half, spot[half], 16:18]

    for hop in range(3):
        for way in range(2):
            for half in range(2):
                if hop < 2 or way == 0:
                    pl.semaphore_wait(token.at[half, way], 1)
                    if hop + way < 2:
                        tell(half, way)

    for step in (4, 3, 5, 2, 6, 1, 7):
        for half in range(2):
            place = (spot[half] + step) % RING
            copy = push(
                meta_tx.at[half, place, pl.ds(0, META)], meta_rx.at[half, spot[half], pl.ds(0, META)],
                send.at[1], recv.at[0], cross[half](step),
            )
            launch(copy)
    send_own(1)

    hub_sum = jnp.zeros((4 * LANES, LANES), jnp.float32)
    for piece in range(2):
        block = jnp.concatenate([ag[half, 0, group, piece] for half in range(2) for group in range(2)], axis=0)
        rows = lax.broadcasted_iota(jnp.int32, (2 * LANES, LANES), 0) + piece * 2 * LANES
        pick = jnp.where(rows == hub_id[...], 1.0, 0.0).astype(jnp.bfloat16)
        hub_sum = hub_sum + dot(split(block), pick)
    hubs[0] = hub_sum[: 2 * LANES] + hub_sum[2 * LANES :]

    def hub_push(index, src, dst, peer):
        launch(push(src, dst, send.at[2], recv.at[index], peer))

    hub_push(1, hubs.at[0], hubs.at[2], along_x(1))
    hub_push(1, hubs.at[0], hubs.at[6], along_x(XS - 1))
    hub_push(3, hubs.at[0], hubs.at[1], partner)

    for copy in large:
        copy.wait()
    tot[...] = jnp.transpose(own[...])

    def relay(wave, group, turn):
        for half in range(2):
            drain(ag_recv.at[half, wave - 1, group, turn], ag.at[half, 0, 0])
            if wave < 3 or turn == 0:
                for way in range(2):
                    launch(table(half, way, wave, group, turn))

    def place_of(half, slot_index):
        return (me[half] + RING - slot_index) % RING

    def lay_counts(slots):
        for half in range(2):
            for slot_index in slots:
                origin = place_of(half, slot_index)
                number = me[1] * RING + origin if half == 0 else origin * RING + me[0]
                lines = lax.broadcasted_iota(jnp.int32, (CAP, LANES), 0) + (HUBS + number * CAP)
                for place in range(RING):
                    count = jnp.zeros((CAP, LANES), jnp.float32)
                    for k in range(FAN):
                        count = count + jnp.where(meta_rx[half, place, k : k + 1] == lines, 1.0, 0.0)
                    top, left = CAP * (place % 4), LANES * (place % 2)
                    cblk[half, slot_index, place // 2, top : top + CAP, left : left + LANES] = count.astype(jnp.bfloat16)

    def add_block(half, slot_index, group):
        block = jnp.concatenate([ag[half, slot_index, group, piece] for piece in range(2)], axis=1)
        wanted = ids[half, pl.ds(place_of(half, slot_index), 1), :]
        rows = lax.broadcasted_iota(jnp.int32, (ROWS, 2 * LANES), 0)
        found = dot(split(block), jnp.where(rows == wanted, 1.0, 0.0).astype(jnp.bfloat16)).astype(jnp.bfloat16)
        for pair in range(RING // 2):
            side = (pair // 2) * LANES
            sums = dot(found[:, side : side + LANES], cblk[half, slot_index, pair])
            sums = sums[:WIDE] + sums[WIDE:]
            for k in range(2):
                piece = sums[:, k * LANES : (k + 1) * LANES]
                if slot_index == 0:
                    pacc[half, 2 * pair + k, group] = piece
                else:
                    pacc[half, 2 * pair + k, group] += piece

    def add_blocks(slots, group):
        for slot_index in slots:
            for half in range(2):
                add_block(half, slot_index, group)

    def hub_block(index, carry):
        chip, over = index // 2, index % 2
        origin = ((me_x + XS - chip) % XS) * 2 + (core + over) % 2
        lines = lax.broadcasted_iota(jnp.int32, (LANES, LANES), 0) + origin * LANES
        mine = spot[0]
        count = jnp.zeros((LANES, LANES), jnp.float32)
        for k in range(FAN):
            count = count + jnp.where(meta_rx[0, mine, k : k + 1] == lines, 1.0, 0.0)
        sums = dot(split(hubs[index]), count.astype(jnp.bfloat16))
        tot[...] += sums[: 2 * LANES] + sums[2 * LANES :]
        return carry

    relay(1, 0, 0)
    relay(1, 0, 1)
    relay(1, 1, 0)
    drain(recv.at[0], meta_rx.at[:, pl.ds(0, RING - 1), pl.ds(0, META)])
    set_of = lax.broadcasted_iota(jnp.int32, (2, LANES), 1) // CAP
    for half in range(2):
        for group in range(2):
            lists = [meta_rx[half, 4 * group + k, 16:18] for k in range(4)]
            for p in range(4):
                row = jnp.zeros((2, LANES), jnp.int32)
                for k in range(4):
                    taken_set = jnp.where(set_of == p, lists[k], 0)
                    row = row + (pltpu.roll(taken_set, ((k - p) % 4) * CAP, 1) if k != p else taken_set)
                ids[half, p : p + 1, group * LANES : (group + 1) * LANES] = row[0:1]
                ids[half, 4 + p : 5 + p, group * LANES : (group + 1) * LANES] = row[1:2]
    lay_counts((0,))
    add_blocks((0,), 0)
    add_blocks((0,), 1)
    relay(1, 1, 1)
    drain(recv.at[1], hubs.at[pl.ds(0, 2)])
    low, high = pl.ds(0, LANES), pl.ds(LANES, LANES)
    hub_push(2, hubs.at[2, low], hubs.at[4, low], along_x(1))
    hub_push(2, hubs.at[6, high], hubs.at[4, high], along_x(XS - 1))
    hub_push(3, hubs.at[2], hubs.at[3], partner)
    hub_push(3, hubs.at[6], hubs.at[7], partner)
    lay_counts((1, 7))
    add_blocks((1, 7), 0)
    relay(2, 0, 0)
    relay(2, 0, 1)
    drain(recv.at[2], hubs.at[0])
    hub_push(3, hubs.at[4], hubs.at[5], partner)
    add_blocks((1, 7), 1)
    lay_counts((2, 6))
    relay(2, 1, 0)
    add_blocks((2, 6), 0)
    relay(3, 0, 0)
    lay_counts((3, 5))
    relay(2, 1, 1)
    relay(3, 0, 1)
    add_blocks((3, 5), 0)
    lay_counts((4,))
    relay(3, 1, 0)
    add_blocks((2, 6), 1)

    def finish(group):
        for half in range(2):
            drain(ag_recv.at[half, 3, group, 0], ag.at[half, 0, 0])
            add_block(half, 4, group)
            here = spot[half]
            for way in range(2):
                sign = 1 - 2 * way
                third = pacc.at[half, (here + 3 * sign + RING) % RING, group]
                fourth = pacc.at[half, (here + 4) % RING, group, pl.ds(way * WIDE // 2, WIDE // 2)]
                launch(
                    push(
                        fourth, far.at[group, half, way, pl.ds(WIDE, WIDE // 2)],
                        send.at[3], far_recv.at[group, half], cross[half]((2 * sign) % RING),
                    )
                )
                launch(
                    push(
                        third, far.at[group, half, way, pl.ds(0, WIDE)],
                        send.at[3], far_recv.at[group, half], cross[half](sign % RING),
                    )
                )
            for way in range(2):
                sign = 1 - 2 * way
                first = pacc.at[half, (here + sign + RING) % RING, group]
                launch(push(first, part.at[group, half, way], send.at[4], recv.at[4 + group], cross[half](sign % RING)))

    def combine(group):
        for half in range(2):
            drain(far_recv.at[group, half], far.at[group, half])
            for way in range(2):
                sign = 1 - 2 * way
                rest = jnp.zeros((WIDE // 2, LANES), jnp.float32)
                piece = far[group, half, way, WIDE:]
                piece = jnp.concatenate([piece, rest] if way == 0 else [rest, piece], axis=0)
                mine = pacc[half, (spot[half] + 2 * sign + RING) % RING, group]
                mix[group, half, way] = mine + far[group, half, way, :WIDE] + piece
                launch(
                    push(
                        mix.at[group, half, way], part.at[group, half, 2 + way],
                        send.at[4], recv.at[4 + group], cross[half]((2 * sign) % RING),
                    )
                )

    finish(0)
    relay(3, 1, 1)
    add_blocks((3, 5), 1)
    finish(1)
    combine(0)
    drain(recv.at[3], hubs.at[pl.ds(0, 4)])
    lax.fori_loop(0, 8, hub_block, 0, unroll=True)
    combine(1)

    product = jnp.zeros((SEEDS, 2 * LANES), jnp.float32)
    for group in range(2):
        drain(recv.at[4 + group], part.at[group])
        lines = []
        for half in range(2):
            top = half * LANES + group * WIDE
            total = tot[top : top + WIDE] + pacc[half, spot[half], group]
            for source in range(4):
                total = total + part[group, half, source]
            lines.append(total)
        mean = jnp.transpose(jnp.concatenate(lines, axis=0) / taken[...])
        parts = [weight[half * LANES + group * WIDE : half * LANES + (group + 1) * WIDE] for half in range(2)]
        product = product + jnp.dot(
            mean, jnp.concatenate(parts, axis=0), precision=lax.Precision.HIGHEST, preferred_element_type=jnp.float32
        )
    out[...] = jnp.maximum(product + bias[...], 0.0)
    drain(send.at[0], ag.at[:, pl.ds(0, RING - 1)])
    drain(send.at[1], meta_tx.at[:, pl.ds(0, RING - 1), pl.ds(0, META)])
    drain(send.at[2], hubs.at[pl.ds(0, 7)])
    drain(send.at[3], far)
    drain(send.at[4], part)


def local(features, seed_self, hub_ids, requests, counts, neighbors, weight, out_bias):
    hbm = pl.BlockSpec(memory_space=pltpu.HBM)
    vmem = pl.BlockSpec(memory_space=pltpu.VMEM)
    dma = pltpu.SemaphoreType.DMA
    return pl.pallas_call(
        kernel,
        out_shape=jax.ShapeDtypeStruct((SEEDS, 2 * LANES), jnp.float32),
        in_specs=[hbm] * 8,
        out_specs=vmem,
        scratch_shapes=[
            pltpu.VMEM((ROWS, 2 * LANES), jnp.float32),
            pltpu.VMEM((SEEDS, 2 * LANES), jnp.float32),
            pltpu.VMEM((1, LANES), jnp.int32),
            pltpu.VMEM((CAP, RING * RING), jnp.int32),
            pltpu.VMEM((RING * RING, CAP), jnp.int32),
            pltpu.SMEM((RING * RING,), jnp.int32),
            pltpu.VMEM((FAN, SEEDS), jnp.int32),
            pltpu.VMEM((2 * LANES, 2 * LANES), jnp.float32),
            pltpu.VMEM((1, 2 * LANES), jnp.float32),
            dma((8,)),
            pltpu.VMEM((2, RING, 2, 2, WIDE, 2 * LANES), jnp.float32),
            pltpu.VMEM((2, RING, 24, LANES), jnp.int32),
            pltpu.VMEM((2, RING, 24, LANES), jnp.int32),
            pltpu.VMEM((2, RING, 2 * LANES), jnp.int32),
            pltpu.VMEM((2, RING, 4, LANES, 2 * LANES), jnp.bfloat16),
            pltpu.VMEM((2, RING, 2, WIDE, LANES), jnp.float32),
            pltpu.VMEM((2, 2, 4, WIDE, LANES), jnp.float32),
            pltpu.VMEM((2, 2, 2, WIDE + WIDE // 2, LANES), jnp.float32),
            pltpu.VMEM((2, 2, 2, WIDE, LANES), jnp.float32),
            pltpu.VMEM((2 * XS, 2 * LANES, LANES), jnp.float32),
            pltpu.VMEM((2 * LANES, LANES), jnp.float32),
            pltpu.VMEM((1, LANES), jnp.float32),
            dma((5,)),
            dma((6,)),
            dma((2, 2)),
            dma((2, 4, 2, 2)),
            pltpu.SemaphoreType.REGULAR((2, 2)),
        ],
        compiler_params=pltpu.CompilerParams(collective_id=0, has_side_effects=True, vmem_limit_bytes=40 * 1024 * 1024),
        name="sage",
    )(
        *(
            pltpu.with_memory_space_constraint(x, pltpu.HBM)
            for x in (
                features, seed_self, hub_ids.reshape(1, LANES), requests.T, counts, neighbors.T, weight,
                out_bias.reshape(1, 2 * LANES),
            )
        )
    )


def solution(mesh):
    rows, flat = P(("rep", "shard"), None), P(("rep", "shard"))
    return jax.shard_map(
        local, mesh=mesh, in_specs=(rows, rows, flat, rows, flat, rows, P(), P()), out_specs=rows, check_vma=False
    )
```
